32 devices in a mesh: pop: 4 (over y, x), dp: 8 (over z, core).
Axes of the slice: x: 2, y: 2, z: 4, core: 2. Of those that a mesh axis runs over, the one named last changes fastest.
Arguments:
- observations: bfloat16 [4, 4096, 256], P('pop', 'dp'), may hold values from -6 to 6
- returns: float32 [4, 4096], P('pop', 'dp'), may hold values from 0 to 2
- actions: int32 [4, 4096], P('pop', 'dp'), may hold values from 0 to 17
- w_input: bfloat16 [4, 256, 2048], P('pop', 'dp'), may hold values from -0.375 to 0.375
- w_middle: bfloat16 [4, 2048, 2048], P('pop', 'dp'), may hold values from -0.125 to 0.125
- w_head: bfloat16 [4, 2048, 18], P('pop', 'dp'), may hold values from -0.125 to 0.125
- log_rate: float32 [4], replicated, may hold values from 3 to 4
- copy_from: int32 [4], replicated, may hold values from 0 to 1, as said below
- perturb: int32 [4], replicated, may hold values from 0 to 2
Outputs:
- next_input: bfloat16 [4, 256, 2048], P('pop', 'dp')
- next_middle: bfloat16 [4, 2048, 2048], P('pop', 'dp')
- next_head: bfloat16 [4, 2048, 18], P('pop', 'dp')
- next_log_rate: float32 [4], P('pop')
- fitness: float32 [4], P('pop')
The draws below stay inside these ranges and needn't reach their ends.
Inputs may be any that keep to these rules, and one draw needn't show every extreme that they name: Some two members that lie 4 apart have copy_from 1.
All inputs are finite; a program needn't handle non-finite values.
Results may differ from the reference program's by a relative error of at most 0.014.
Values may be sent and summed in bfloat16 or wider, within the bound.
No kernel may reach another device: no remote copies, remote signals or barrier semaphores. Data moves between devices by JAX's collectives and lax.ppermute only.
A program may use at most 128 MiB of HBM per device.

```python
import jax
import jax.numpy as jnp
from jax import lax

D = 2048
OBS = 256
ACT = 18
ROWS_DEV = 512
POP = 4
BATCH = 4096
N_DP = 8


def draw_copy_from(key, part):
    marks = jax.random.randint(jax.random.fold_in(key, 23), (POP,), 0, 2).astype(jnp.int32)
    turn = jax.random.randint(jax.random.fold_in(key, 41), (), 0, POP).astype(jnp.int32)
    members = jnp.arange(POP, dtype=jnp.int32)
    forced = (members == turn) | (members == (turn + POP // 2) % POP)
    return jnp.where(forced, 1, marks).astype(jnp.int32)


def with_ends(drawn, own_key, least, high):
    longest = drawn.shape.index(max(drawn.shape))
    spots = []
    for shift in (0, 1):
        where = [jax.random.randint(jax.random.fold_in(own_key, axis), (), 0, length) for axis, length in enumerate(drawn.shape)]
        where[longest] = (where[longest] + shift) % drawn.shape[longest]
        spots.append(tuple(where))
    return drawn.at[spots[0]].set(least).at[spots[1]].set(high)


def block_levels(own_key, shape, shards, smallest, largest):
    def one(axis_at, blocks):
        steps = jax.random.uniform(jax.random.fold_in(jax.random.fold_in(own_key, 6), axis_at), (blocks,), jnp.float32, smallest / len(shards), largest / len(shards))
        return jnp.repeat(jnp.exp(steps), shape[axis_at] // blocks).reshape((-1,) + (1,) * (len(shape) - axis_at - 1))

    gain = one(*shards[0])
    for cut in shards[1:]:
        gain = gain * one(*cut)
    return gain


def centred(own_key, dims, width, most, split=(), kind=jnp.bfloat16):
    loudness = block_levels(own_key, dims, split, -0.22, 0.18) if split else 1.0
    values = jax.random.normal(own_key, dims, jnp.float32) * width * loudness
    return jnp.minimum(jnp.maximum(values, -most), most).astype(kind)


def setup_inputs(seed: int = 0) -> dict:
    arg_keys = jax.random.split(jax.random.key(seed), 10)
    observations = centred(arg_keys[0], (POP, BATCH, OBS), 1.0, 6.0, ((0, 4), (1, 8)))
    returns = jnp.clip(2.0 * jax.random.uniform(arg_keys[1], (POP, BATCH), jnp.float32) ** block_levels(arg_keys[1], (POP, BATCH), ((0, 4), (1, 8)), -0.2, 0.2), 0.0, 2.0)
    actions = with_ends(jax.random.randint(arg_keys[2], (POP, BATCH), 0, ACT), jax.random.fold_in(arg_keys[2], 1), 0, ACT - 1).astype(jnp.int32)
    w_input = centred(arg_keys[3], (POP, OBS, D), OBS ** -0.5, 0.375, ((0, 4), (1, 8)))
    w_middle = centred(arg_keys[4], (POP, D, D), D ** -0.5, 0.125, ((0, 4), (1, 8)))
    w_head = centred(arg_keys[5], (POP, D, ACT), D ** -0.5, 0.125, ((0, 4), (1, 8)))
    log_rate = jnp.clip(jax.random.uniform(arg_keys[6], (POP,), jnp.float32, 3.0, 4.0), 3.0, 4.0)
    copy_from = draw_copy_from(jax.random.fold_in(arg_keys[9], 71), 0)
    perturb = with_ends(jax.random.randint(arg_keys[8], (POP,), 0, 3), jax.random.fold_in(arg_keys[8], 1), 0, 2).astype(jnp.int32)
    return dict(observations=observations, returns=returns, actions=actions, w_input=w_input, w_middle=w_middle, w_head=w_head, log_rate=log_rate, copy_from=copy_from, perturb=perturb)


CAP = 2.0


def silu_slope(pre):
    sig = jax.nn.sigmoid(pre)
    return sig * (1.0 + pre * (1.0 - sig))


def rounded(value):
    return lax.optimization_barrier(value.astype(jnp.bfloat16)).astype(jnp.float32)


def member_step(member):
    obs, gains, chosen, first, middle, head, rate = member
    pre1 = jnp.dot(obs, first, preferred_element_type=jnp.float32)
    hidden1 = jax.nn.silu(pre1).astype(jnp.bfloat16)
    pre2 = jnp.dot(hidden1, middle, preferred_element_type=jnp.float32)
    hidden2 = jax.nn.silu(pre2).astype(jnp.bfloat16)
    squash = jnp.tanh(jnp.dot(hidden2, head, preferred_element_type=jnp.float32) / CAP)
    logits = CAP * squash
    logp = logits - jnp.log(jnp.sum(jnp.exp(logits), axis=1, keepdims=True))
    onehot = (chosen[:, None] == lax.broadcasted_iota(jnp.int32, logits.shape, 1)).astype(jnp.float32)
    taken = jnp.sum(logp * onehot, axis=1)
    fitness = jnp.sum(gains * taken) / BATCH
    grad_raw = (-(gains / BATCH)[:, None] * (onehot - jnp.exp(logp)) * (1.0 - squash * squash)).astype(jnp.bfloat16)
    grad_pre2 = (jnp.dot(grad_raw, head.T, preferred_element_type=jnp.float32) * silu_slope(pre2)).astype(jnp.bfloat16)
    grad_pre1 = (jnp.dot(grad_pre2, middle.T, preferred_element_type=jnp.float32) * silu_slope(pre1)).astype(jnp.bfloat16)

    def add_block(carry, parts):
        obs_b, grad1_b, hid1_b, grad2_b, hid2_b, graw_b = parts
        total1, total2, total3 = carry
        total1 = total1 + rounded(jnp.dot(obs_b.T, grad1_b, preferred_element_type=jnp.float32))
        total2 = total2 + rounded(jnp.dot(hid1_b.T, grad2_b, preferred_element_type=jnp.float32))
        total3 = total3 + rounded(jnp.dot(hid2_b.T, graw_b, preferred_element_type=jnp.float32))
        return (total1, total2, total3), None

    blocks = tuple(part.reshape(N_DP, ROWS_DEV, part.shape[1]) for part in (obs, grad_pre1, hidden1, grad_pre2, hidden2, grad_raw))
    start = (jnp.zeros(first.shape, jnp.float32), jnp.zeros(middle.shape, jnp.float32), jnp.zeros(head.shape, jnp.float32))
    (grad_first, grad_middle, grad_head), unused = lax.scan(add_block, start, blocks)
    new_first = (first.astype(jnp.float32) - rate * grad_first).astype(jnp.bfloat16)
    new_middle = (middle.astype(jnp.float32) - rate * grad_middle).astype(jnp.bfloat16)
    new_head = (head.astype(jnp.float32) - rate * grad_head).astype(jnp.bfloat16)
    return new_first, new_middle, new_head, fitness


def reference(observations, returns, actions, w_input, w_middle, w_head, log_rate, copy_from, perturb):
    rates = jnp.exp(log_rate)
    new_first, new_middle, new_head, fitness = lax.map(member_step, (observations, returns, actions, w_input, w_middle, w_head, rates))
    flag = copy_from == 1
    next_input = jnp.where(flag[:, None, None], jnp.roll(new_first, 1, axis=0), new_first)
    next_middle = jnp.where(flag[:, None, None], jnp.roll(new_middle, 1, axis=0), new_middle)
    next_head = jnp.where(flag[:, None, None], jnp.roll(new_head, 1, axis=0), new_head)
    members = jnp.arange(POP, dtype=jnp.int32)
    source = jnp.where(flag, (members + POP - 1) % POP, members)
    offset = jnp.where(perturb == 0, -0.2, jnp.where(perturb == 1, 0.0, 0.2)).astype(jnp.float32)
    next_log_rate = log_rate[source] + offset
    return next_input, next_middle, next_head, next_log_rate, fitness
```

```python
import jax
import jax.numpy as jnp
from jax import lax
from jax.experimental import pallas as pl
from jax.experimental.pallas import tpu as pltpu
from jax.sharding import PartitionSpec as P

CAP = 2.0
CHUNKS = 4
GROUPS = 2


def silu_slope(pre):
    sig = jax.nn.sigmoid(pre)
    return sig * (1.0 + pre * (1.0 - sig))


def contract_rows(left, right):
    return lax.dot_general(
        left, right, (((0,), (0,)), ((), ())), preferred_element_type=jnp.float32
    )


def contract_cols(left, right):
    return lax.dot_general(
        left, right, (((1,), (1,)), ((), ())), preferred_element_type=jnp.float32
    )


def sigmoid(v):
    return 0.5 + 0.5 * jnp.tanh(0.5 * v)


def dot(left, right, dims=((1,), (0,))):
    return lax.dot_general(left, right, (dims, ((), ())), preferred_element_type=jnp.float32)


def params(mib, *semantics):
    return pltpu.CompilerParams(dimension_semantics=semantics or None, vmem_limit_bytes=mib << 20)


def hbm(array):
    return pltpu.with_memory_space_constraint(array, pltpu.HBM)


def whole(array):
    return pl.BlockSpec(array.shape, lambda *_: (0,) * array.ndim)


def cost(flops, moved):
    return pl.CostEstimate(flops=int(flops), bytes_accessed=int(moved), transcendentals=0)


def first_layer(order, pieces, theirs, rows, slab, near_blocks):
    count = len(pieces)
    devices = 2 * count
    features = pieces[0].shape[1]
    each = features // devices
    mids = devices * each
    pad_acts = pieces[0].shape[0] - rows - mids
    width = devices * slab
    total = count * rows
    near_all = 2 * near_blocks

    def near_at(i):
        return (i // count) * near_blocks + jnp.minimum(i % count, near_blocks - 1)

    def kernel(order_ref, *refs):
        piece_refs, theirs_ref = refs[:count], refs[count]
        h1_ref, h1t_ref, slope_ref, obst_ref, head_ref, cols = refs[count + 1 :]
        i = pl.program_id(0)

        def small(k, start, size):
            if k < count:
                return piece_refs[k][pl.ds(rows + start, size), :]
            return theirs_ref[k - count, pl.ds(start, size), :]

        @pl.when(i == 0)
        def _():
            for k in range(devices):
                at = pl.multiple_of(order_ref[k] * each, each)
                lanes = pl.multiple_of(order_ref[k] * slab, slab)
                head_ref[:, pl.ds(lanes, slab)] = small(k, mids, pad_acts)
                for b in range(devices):
                    source = pl.multiple_of(order_ref[b] * each, each)
                    cols[b, pl.ds(at, each), :] = small(k, source, each)
            for p in range(count):
                block = piece_refs[p][:rows, :].astype(jnp.float32)
                obst_ref[:, p * rows : (p + 1) * rows] = block.T.astype(jnp.bfloat16)

        weights = cols[i]
        for p in range(count):
            pre = dot(piece_refs[p][:rows, :], weights)
            h1_ref[p * rows : (p + 1) * rows, :] = (pre * sigmoid(pre)).astype(jnp.bfloat16)

        @pl.when(i % count < near_blocks)
        def _():
            for p in range(count):
                obs = piece_refs[p][:rows, :]
                pre = dot(obs, weights)
                sig = sigmoid(pre)
                slope_ref[p * rows : (p + 1) * rows, :] = (sig * (1.0 + pre * (1.0 - sig))).astype(jnp.bfloat16)
                pre_t = dot(weights, obs, ((0,), (1,)))
                h1t_ref[:, p * rows : (p + 1) * rows] = (pre_t * sigmoid(pre_t)).astype(jnp.bfloat16)

    shape = lambda *s: jax.ShapeDtypeStruct(s, jnp.bfloat16)
    return pl.pallas_call(
        kernel,
        name="first_layer",
        grid_spec=pltpu.PrefetchScalarGridSpec(
            num_scalar_prefetch=1,
            grid=(devices,),
            in_specs=[whole(p) for p in pieces] + [whole(theirs)],
            out_specs=[
                pl.BlockSpec((total, slab), lambda i, _: (0, i)),
                pl.BlockSpec((slab, total), lambda i, _: (near_at(i), 0)),
                pl.BlockSpec((total, slab), lambda i, _: (0, near_at(i))),
                pl.BlockSpec((features, total), lambda i, _: (0, 0)),
                pl.BlockSpec((pad_acts, width), lambda i, _: (0, 0)),
            ],
            scratch_shapes=[pltpu.VMEM((devices, features, slab), jnp.bfloat16)],
        ),
        out_shape=[
            shape(total, width),
            shape(near_all * slab, total),
            pltpu.HBM((total, near_all * slab), jnp.bfloat16),
            pltpu.HBM((features, total), jnp.bfloat16),
            shape(pad_acts, width),
        ],
        cost_estimate=cost(2 * total * features * width * 2, 30 << 20),
        compiler_params=params(20, "arbitrary"),
    )(order, *map(hbm, pieces), hbm(theirs))


def second_layer(hidden1, own, pieces, theirs, head, logits, hidden2, q, cut):
    total, width = hidden1.shape
    slab = own.shape[0]
    pad_acts = head.shape[0]
    tile = min(512, total)
    first = logits is None
    sub = 256

    def kernel(h1_ref, own_ref, *refs):
        piece_refs = refs[: len(pieces)]
        theirs_ref, head_ref = refs[len(pieces) : len(pieces) + 2]
        rest = refs[len(pieces) + 2 :]
        logits_in = None if first else rest[0]
        h2_ref, slope_ref, logits_ref, weights = rest[0 if first else 2 :]

        @pl.when(pl.program_id(0) == 0)
        def _():
            weights[:slab] = own_ref[...]
            for k, piece in enumerate(piece_refs):
                weights[(k + 1) * slab : (k + 2) * slab] = piece[...]
            weights[(len(pieces) + 1) * slab :] = theirs_ref[...]

        for r in range(0, tile, sub):
            pre = dot(h1_ref[r : r + sub, :], weights[...])
            sig = sigmoid(pre)
            hidden = (pre * sig).astype(jnp.bfloat16)
            h2_ref[r : r + sub, :] = hidden
            slope_ref[r : r + sub, :] = (sig * (1.0 + pre * (1.0 - sig))).astype(jnp.bfloat16)
            part = dot(hidden, head_ref[...], ((1,), (1,)))
            logits_ref[r : r + sub, :] = part if first else part + logits_in[r : r + sub, :]

    row = lambda size: pl.BlockSpec((tile, size), lambda i: (i, 0))
    return pl.pallas_call(
        kernel,
        name="second_layer",
        grid=(total // tile,),
        in_specs=[row(width), pl.BlockSpec((slab, cut), lambda i: (0, q))]
        + [whole(p) for p in pieces]
        + [whole(theirs), pl.BlockSpec((pad_acts, cut), lambda i: (0, q))]
        + ([] if first else [row(pad_acts), pl.BlockSpec(memory_space=pltpu.HBM)]),
        out_specs=[pl.BlockSpec((tile, cut), lambda i: (i, q)), row(cut), row(pad_acts)],
        out_shape=[
            pltpu.HBM((total, width), jnp.bfloat16),
            jax.ShapeDtypeStruct((total, cut), jnp.bfloat16),
            jax.ShapeDtypeStruct((total, pad_acts), jnp.float32),
        ],
        scratch_shapes=[pltpu.VMEM((width, cut), jnp.bfloat16)],
        input_output_aliases={} if first else {len(pieces) + 5: 0},
        cost_estimate=cost(2 * total * width * cut, 16 << 20),
        compiler_params=params(18, "arbitrary"),
    )(hidden1, hbm(own), *map(hbm, pieces), hbm(theirs), head, *([] if first else [logits, hbm(hidden2)]))


def policy(logits_raw, labels, acts, batch):
    total, pad_acts = logits_raw.shape

    def kernel(raw_ref, labels_ref, graw_ref, graw_t_ref, score_ref):
        raw = raw_ref[...].T
        gains, chosen = labels_ref[0:1, :], labels_ref[1:2, :].astype(jnp.int32)
        at = lax.broadcasted_iota(jnp.int32, raw.shape, 0)
        live = at < acts
        squash = jnp.tanh(raw / CAP)
        logits = CAP * squash
        mass = jnp.sum(jnp.where(live, jnp.exp(logits), 0.0), axis=0, keepdims=True)
        logp = logits - jnp.log(mass)
        onehot = at == chosen
        taken = jnp.sum(jnp.where(onehot, logp, 0.0), axis=0, keepdims=True)
        score_ref[...] = jnp.sum(gains * taken, axis=1, keepdims=True) / batch
        grad = -(gains / batch) * (onehot.astype(jnp.float32) - jnp.exp(logp)) * (1.0 - squash * squash)
        grad = jnp.where(live, grad, 0.0)
        graw_t_ref[...] = grad.astype(jnp.bfloat16)
        graw_ref[...] = grad.T.astype(jnp.bfloat16)

    return pl.pallas_call(
        kernel,
        name="policy",
        out_shape=[
            jax.ShapeDtypeStruct((total, pad_acts), jnp.bfloat16),
            jax.ShapeDtypeStruct((pad_acts, total), jnp.bfloat16),
            jax.ShapeDtypeStruct((1, 1), jnp.float32),
        ],
        cost_estimate=cost(1 << 28, 2 << 20),
        compiler_params=params(10),
    )(logits_raw, labels)


def middle_grad(graw, head, slopes, hidden1_t, first, cut):
    total, pad_acts = graw.shape
    near_rows = hidden1_t.shape[0]
    kept = near_rows // 2
    tile = min(256, kept)
    steps = near_rows // tile
    parts = len(slopes)
    span = parts * cut

    def kernel(graw_ref, head_ref, *refs):
        slope_refs = refs[:parts]
        h1t_ref, g2_ref, keep_ref, give_ref = refs[parts:]
        i = pl.program_id(0)

        @pl.when(i == 0)
        def _():
            for p in range(parts):
                lanes = slice(p * cut, (p + 1) * cut)
                for r in range(0, total, 256):
                    g2 = dot(graw_ref[r : r + 256, :], head_ref[:, lanes]) * slope_refs[p][r : r + 256, :].astype(jnp.float32)
                    g2_ref[r : r + 256, lanes] = g2.astype(jnp.bfloat16)

        part = dot(h1t_ref[...], g2_ref[...])

        @pl.when(i < steps // 2)
        def _():
            give_ref[...] = part.astype(jnp.bfloat16)

        @pl.when(i >= steps // 2)
        def _():
            keep_ref[...] = part

    turn = lambda i: (i + steps // 2) % steps
    return pl.pallas_call(
        kernel,
        name="middle_grad",
        grid=(steps,),
        in_specs=[whole(graw), pl.BlockSpec((pad_acts, span), lambda i: (0, first // parts))]
        + [whole(v) for v in slopes]
        + [pl.BlockSpec((tile, total), lambda i: (turn(i), 0))],
        out_specs=[
            pl.BlockSpec((total, span), lambda i: (0, 0)),
            pl.BlockSpec((tile, span), lambda i: (jnp.maximum(i - steps // 2, 0), 0)),
            pl.BlockSpec((tile, span), lambda i: (jnp.minimum(i, steps // 2 - 1), 0)),
        ],
        out_shape=[
            jax.ShapeDtypeStruct((total, span), jnp.bfloat16),
            jax.ShapeDtypeStruct((kept, span), jnp.float32),
            pltpu.HBM((kept, span), jnp.bfloat16),
        ],
        cost_estimate=cost(2 * total * near_rows * span, 16 << 20),
        compiler_params=params(24, "arbitrary"),
    )(graw, head, *slopes, hidden1_t)


def head_grad(scalars, graw_t, hidden2):
    pad_acts, total = graw_t.shape
    side = hidden2.shape[1] // 2
    block = min(512, side)

    def kernel(scalar_ref, graw_t_ref, h2_ref, out_ref):
        out_ref[...] = dot(graw_t_ref[...], h2_ref[...])

    return pl.pallas_call(
        kernel,
        name="head_grad",
        grid_spec=pltpu.PrefetchScalarGridSpec(
            num_scalar_prefetch=1,
            grid=(side // block,),
            in_specs=[
                pl.BlockSpec((pad_acts, total), lambda i, _: (0, 0)),
                pl.BlockSpec((total, block), lambda i, s: (0, s[1] * (side // block) + i)),
            ],
            out_specs=pl.BlockSpec((pad_acts, block), lambda i, _: (0, i)),
        ),
        out_shape=jax.ShapeDtypeStruct((pad_acts, side), jnp.float32),
        cost_estimate=cost(2 * total * side * 256, 6 << 20),
        compiler_params=params(10, "arbitrary"),
    )(scalars, graw_t, hbm(hidden2))


def middle_update(rate, keep, got, own, near_pieces, group, span, cut):
    slab = own.shape[0]
    per = span // cut
    blocks = 1 + len(near_pieces[0])
    flat = [p for chunk in near_pieces for p in chunk]

    def kernel(rate_ref, keep_ref, got_ref, own_ref, *refs):
        flat_refs, out_refs = refs[: len(flat)], refs[len(flat) :]
        rate = rate_ref[0:1, 0:1]
        for s in reversed(range(blocks)):
            for p in range(per):
                lanes, at = slice(p * cut, (p + 1) * cut), slice(s * slab, (s + 1) * slab)
                weight = own_ref[:, lanes] if s == 0 else flat_refs[p * (blocks - 1) + s - 1][...]
                total = keep_ref[at, lanes] + got_ref[at, lanes].astype(jnp.float32)
                out_refs[s][:, lanes] = (weight.astype(jnp.float32) - rate * total).astype(jnp.bfloat16)

    return pl.pallas_call(
        kernel,
        name="middle_update",
        grid=(1,),
        in_specs=[whole(rate), whole(keep), whole(got)]
        + [pl.BlockSpec((slab, span), lambda i: (0, group))]
        + [whole(p) for p in flat],
        out_specs=[pl.BlockSpec((slab, span), lambda i: (0, 0))] * blocks,
        out_shape=[pltpu.HBM((slab, span), jnp.bfloat16)] * blocks,
        cost_estimate=cost(1 << 27, 4 << 20),
        compiler_params=params(16, "arbitrary"),
    )(rate, keep, hbm(got), hbm(own), *map(hbm, flat))


def gather_small(scalars, order, keep, got, side, score, first_rows, slab, half):
    count = 2 * half
    devices = 2 * count
    mids = devices * first_rows
    pad_acts = side.shape[0]
    acts_at = mids + pad_acts

    def kernel(scalar_ref, order_ref, keep_ref, got_ref, side_ref, score_ref, mine_ref, sent_ref):
        core = scalar_ref[0]
        for target, which in ((sent_ref, 1 - core), (mine_ref, core)):
            for j in range(half):
                base = pl.multiple_of(j * 2 * first_rows + which * first_rows, first_rows)
                for k in range(devices):
                    source = got_ref if (k // half) % 2 else keep_ref
                    lanes = ((k // count) * half + k % half) * slab
                    at = pl.multiple_of(order_ref[k] * first_rows, first_rows)
                    target[j, pl.ds(at, first_rows), :] = source[pl.ds(base, first_rows), lanes : lanes + slab]
                cols = pl.multiple_of((j * 2 + which) * slab, slab)
                target[j, mids:acts_at, :] = side_ref[:, pl.ds(cols, slab)].astype(jnp.bfloat16)
        value = jnp.broadcast_to(score_ref[...], (1, slab))
        for part in range(3):
            piece = value.astype(jnp.bfloat16)
            sent_ref[0, acts_at - 3 + part : acts_at - 2 + part, :] = piece
            value = value - piece.astype(jnp.float32)

    shape = jax.ShapeDtypeStruct((half, acts_at, slab), jnp.bfloat16)
    smem = pl.BlockSpec(memory_space=pltpu.SMEM)
    arrays = [keep, hbm(got), side, score]
    return pl.pallas_call(
        kernel,
        name="gather_small",
        grid=(1,),
        in_specs=[smem, smem] + [whole(v) for v in arrays],
        out_specs=[whole(shape)] * 2,
        out_shape=[shape, pltpu.HBM(shape.shape, shape.dtype)],
        cost_estimate=cost(1 << 26, 2 << 20),
        compiler_params=params(8, "arbitrary"),
    )(scalars, order, *arrays)


def small_update(scalars, rate, mine, got, weights, score):
    half, rows, slab = mine.shape

    def kernel(scalar_ref, rate_ref, mine_ref, got_ref, *refs):
        weight_refs = refs[:half]
        score_ref, fitness_ref = refs[half], refs[half + 1]
        out_refs = refs[half + 2 :]
        rate, high = rate_ref[0:1, 0:1], scalar_ref[1]
        fitness = jnp.broadcast_to(score_ref[...], (1, slab))
        for part in range(3):
            fitness = fitness + got_ref[0, rows - 3 + part : rows - 2 + part, :].astype(jnp.float32)
        fitness_ref[...] = fitness[:, :1]
        for s in range(half):
            at = jnp.where(high == 1, s, half - 1 - s)
            total = mine_ref[at].astype(jnp.float32) + got_ref[at].astype(jnp.float32)
            out_refs[s][...] = (weight_refs[s][-rows:, :].astype(jnp.float32) - rate * total).astype(jnp.bfloat16)
            value = fitness
            for part in range(3):
                piece = value.astype(jnp.bfloat16)
                out_refs[s][rows - 3 + part : rows - 2 + part, :] = piece
                value = value - piece.astype(jnp.float32)

    smem = pl.BlockSpec(memory_space=pltpu.SMEM)
    return pl.pallas_call(
        kernel,
        name="small_update",
        grid=(1,),
        in_specs=[smem] + [whole(v) for v in (rate, mine, got, *weights, score)],
        out_specs=[pl.BlockSpec((1, 1), lambda i: (0, 0))] + [pl.BlockSpec((rows, slab), lambda i: (0, 0))] * half,
        out_shape=[jax.ShapeDtypeStruct((1, 1), jnp.float32)] + [pltpu.HBM((rows, slab), jnp.bfloat16)] * half,
        cost_estimate=cost(1 << 26, 2 << 20),
        compiler_params=params(8, "arbitrary"),
    )(scalars, rate, mine, hbm(got), *map(hbm, weights), score)


def input_grad(scalars, grads, own, near_pieces, theirs, slope, obs_t, cut):
    total = grads[0].shape[0]
    slab, width = own.shape
    near_rows = slope.shape[1]
    kept = near_rows // 2
    features = obs_t.shape[0]
    groups = len(grads)
    chunks = len(theirs)
    side = features // 2
    tile = min(256, total)
    flat = [p for chunk in near_pieces for p in chunk]
    per = len(flat) // chunks

    def kernel(scalar_ref, *refs):
        g_refs, refs = refs[:groups], refs[groups:]
        own_ref, refs = refs[0], refs[1:]
        flat_refs, refs = refs[: len(flat)], refs[len(flat) :]
        theirs_refs, refs = refs[:chunks], refs[chunks:]
        slope_ref, obst_ref, keep_ref, give_ref, weights, total_ref = refs
        i = pl.program_id(0)

        @pl.when(i == 0)
        def _():
            weights[:slab] = own_ref[...]
            for q in range(chunks):
                lanes = slice(q * cut, (q + 1) * cut)
                for k in range(per):
                    weights[(k + 1) * slab : (k + 2) * slab, lanes] = flat_refs[q * per + k][...]
                weights[kept:, lanes] = theirs_refs[q][...]
            total_ref[...] = jnp.zeros_like(total_ref)

        g2 = jnp.concatenate([g[...] for g in g_refs], axis=1)
        back = dot(g2, weights[...], ((1,), (1,)))
        grad = (back * slope_ref[...].astype(jnp.float32)).astype(jnp.bfloat16)
        total_ref[...] += dot(obst_ref[...], grad)

        @pl.when(i == pl.num_programs(0) - 1)
        def _():
            high = scalar_ref[1]
            keep_ref[...] = total_ref[pl.ds(pl.multiple_of(high * side, side), side), :].astype(jnp.bfloat16)
            give_ref[...] = total_ref[pl.ds(pl.multiple_of((1 - high) * side, side), side), :].astype(jnp.bfloat16)

    return pl.pallas_call(
        kernel,
        name="input_grad",
        grid=(total // tile,),
        in_specs=[pl.BlockSpec(memory_space=pltpu.SMEM)]
        + [pl.BlockSpec((tile, g.shape[1]), lambda i: (i, 0)) for g in grads]
        + [whole(own)]
        + [whole(p) for p in flat]
        + [pl.BlockSpec((kept, cut), lambda i: (0, 0))] * chunks
        + [pl.BlockSpec((tile, near_rows), lambda i: (i, 0)), pl.BlockSpec((features, tile), lambda i: (0, i))],
        out_specs=[pl.BlockSpec((side, near_rows), lambda i: (0, 0))] * 2,
        out_shape=[
            jax.ShapeDtypeStruct((side, near_rows), jnp.bfloat16),
            pltpu.HBM((side, near_rows), jnp.bfloat16),
        ],
        scratch_shapes=[
            pltpu.VMEM((near_rows, width), jnp.bfloat16),
            pltpu.VMEM((features, near_rows), jnp.float32),
        ],
        cost_estimate=cost(2 * total * near_rows * width, 20 << 20),
        compiler_params=params(26, "arbitrary"),
    )(scalars, *grads, hbm(own), *map(hbm, flat), *map(hbm, theirs), hbm(slope), hbm(obs_t))


def settings(numbers, log_rate, copy_from, perturb, devices):
    members = log_rate.shape[0]

    def kernel(numbers_ref, log_rate_ref, copy_ref, perturb_ref, order_ref, scalars_ref, rate_ref, flag_ref, next_ref):
        for k in range(devices):
            order_ref[k] = numbers_ref[k]
        for k in range(2):
            scalars_ref[k] = numbers_ref[devices + k]
        member = numbers_ref[devices + 2]
        rate_ref[...] = jnp.exp(jnp.full(rate_ref.shape, log_rate_ref[member], jnp.float32))
        taken = copy_ref[member] == 1
        flag_ref[0] = taken.astype(jnp.int32)
        source = jnp.where(taken, lax.rem(member + members - 1, members), member)
        pick = perturb_ref[member]
        offset = jnp.where(pick == 0, -0.2, jnp.where(pick == 1, 0.0, 0.2)).astype(jnp.float32)
        next_ref[...] = jnp.full(next_ref.shape, log_rate_ref[source] + offset, jnp.float32)

    smem = pl.BlockSpec(memory_space=pltpu.SMEM)
    vmem = pl.BlockSpec(memory_space=pltpu.VMEM)
    ints = lambda n: jax.ShapeDtypeStruct((n,), jnp.int32)
    return pl.pallas_call(
        kernel,
        name="settings",
        in_specs=[smem] * 4,
        out_specs=[smem, smem, vmem, smem, vmem],
        out_shape=[
            ints(devices),
            ints(2),
            jax.ShapeDtypeStruct((8, 128), jnp.float32),
            ints(1),
            jax.ShapeDtypeStruct((1, 1), jnp.float32),
        ],
        cost_estimate=cost(1 << 10, 1 << 10),
        compiler_params=params(4),
    )(numbers, log_rate, copy_from, perturb)


def hub_body(observations, returns, actions, w_input, w_middle, w_head, log_rate, copy_from, perturb):
    obs, gains, chosen = observations[0], returns[0], actions[0]
    own_first, own_middle, own_head = w_input[0], w_middle[0], w_head[0]
    devices = lax.axis_size("dp")
    half = devices // 4
    count = 2 * half
    rows, _ = obs.shape
    first_rows, width = own_first.shape
    slab = own_middle.shape[0]
    acts = own_head.shape[1]
    pad_acts = -(-(acts + 3) // 32) * 32
    batch = rows * devices
    mids = devices * first_rows
    cut = width // CHUNKS
    place = lax.axis_index("dp")
    core = place % 2
    chip = place // 2
    high = (chip >= half).astype(jnp.int32)
    member = lax.axis_index("pop")
    members = lax.axis_size("pop")
    ring = [(i, (i + 1) % members) for i in range(members)]

    def side(step, upper):
        return half + step if upper else half - 1 - step

    def route(step, crossing, back=False):
        pairs = []
        for upper in (False, True):
            hub = side(0, upper != crossing)
            end = side(step, upper)
            pairs += [(2 * end + c, 2 * hub + c) for c in range(2)]
        return [(b, a) for a, b in pairs] if back else pairs

    def near(value, step):
        return lax.ppermute(value, "dp", route(step, False))

    def far(value, step):
        return lax.ppermute(value, "dp", route(step, True))

    def outward(value, step):
        return lax.ppermute(value, "dp", route(step, False, True))

    def partner(value):
        return lax.ppermute(value, "dp", [(i, i ^ 1) for i in range(devices)])

    def shifted(value):
        return lax.ppermute(value, "pop", ring)

    slots = jnp.arange(devices, dtype=jnp.int32)
    upper = high ^ ((slots // half) % 2)
    order = 2 * jnp.where(upper == 1, half + slots % half, half - 1 - slots % half) + (core ^ (slots // count))

    numbers = jnp.concatenate([order, jnp.stack([core, high, member])]).astype(jnp.int32)
    order, scalars, rate, flag, next_rate = settings(numbers, log_rate, copy_from, perturb, devices)

    def column(value):
        out = []
        for s in range(1, half):
            out.append(near(value, s))
        for s in range(half):
            out.append(far(value, s))
        return out

    packed = jnp.concatenate(
        [
            obs,
            own_first.reshape(first_rows, devices, slab).swapaxes(0, 1).reshape(-1, slab),
            jnp.pad(own_head.T, ((0, pad_acts - acts), (0, 0))),
        ],
        axis=0,
    )
    pieces = [packed] + column(packed)
    middle_pieces = [column(own_middle[:, q * cut : (q + 1) * cut]) for q in range(CHUNKS)]
    labels = jnp.stack([gains, chosen.astype(jnp.float32)])
    labels = jnp.concatenate([labels] + column(labels), axis=1)
    theirs_small = partner(jnp.stack([p[rows:] for p in pieces]))
    hidden1, near_t, slope1, obs_t, head = first_layer(order, pieces, theirs_small, rows, slab, half)

    logits = None
    hidden2, slope2, theirs = None, [], []
    for q in range(CHUNKS):
        mine = jnp.concatenate([own_middle[:, q * cut : (q + 1) * cut]] + middle_pieces[q], axis=0)
        theirs.append(partner(mine))
        hidden2, slope, logits = second_layer(
            hidden1, own_middle, middle_pieces[q], theirs[q], head, logits, hidden2, q, cut
        )
        slope2.append(slope)

    grad_raw, grad_raw_t, score = policy(logits, labels, acts, batch)

    distance = jnp.where(high == 1, chip - half, half - 1 - chip)

    def home(blocks):
        out = blocks[0]
        for s in range(1, half):
            moved = outward(blocks[s], s)
            out = jnp.where(distance == s, moved, out)
        return out

    flag = flag[0] == 1

    near_w = [m[: half - 1] for m in middle_pieces]
    per = CHUNKS // GROUPS
    span = per * cut
    out_middle, grads = [], []
    for g in range(GROUPS):
        part = slice(g * per, (g + 1) * per)
        g2, keep, give = middle_grad(grad_raw, head, slope2[part], near_t, g * per, cut)
        got = partner(give)
        new = middle_update(rate, keep, got, own_middle, near_w[part], g, span, cut)
        new = home(new)
        moved = shifted(new)
        out_middle.append(jnp.where(flag, moved, new))
        grads.append(g2)
    out_middle = jnp.concatenate(out_middle, axis=1)

    keep, give = input_grad(scalars, grads, own_middle, near_w, theirs, slope1, obs_t, cut)
    got = far(give, 0)
    head_term = head_grad(scalars, grad_raw_t, hidden2)
    mine, sent = gather_small(scalars, order, keep, got, head_term, score, first_rows, slab, half)
    got = partner(sent)
    fitness, *new_small = small_update(scalars, rate, mine, got, pieces[:half], score)
    new_small = home(new_small)
    fitness = jnp.where(
        distance == 0, fitness, jnp.sum(new_small[-3:, :1].astype(jnp.float32), axis=0, keepdims=True)
    )
    moved = shifted(new_small)
    out_small = jnp.where(flag, moved, new_small)
    out_first = out_small[:mids].reshape(devices, first_rows, slab).swapaxes(0, 1).reshape(first_rows, width)
    out_head = out_small[mids : mids + acts].T

    return (
        out_first[None],
        out_middle[None],
        out_head[None],
        next_rate.reshape(1),
        fitness.reshape(1),
    )


def hub_step(*arrays):
    return hub_body(*arrays)


def shifted(block, axis, distance):
    devices = range(lax.axis_size(axis))
    route = [((i - distance) % len(devices), i) for i in devices]
    return lax.ppermute(block, axis, route)


def local(observations, returns, actions, w_input, w_middle, w_head, log_rate, copy_from, perturb):
    obs = observations[0]
    gains = returns[0]
    chosen = actions[0]
    own_first = w_input[0]
    own_middle = w_middle[0]
    own_head = w_head[0]
    rows = obs.shape[0]
    batch = rows * lax.axis_size("dp")
    first, head = (
        lax.all_gather(own_first, "dp", axis=0, tiled=True),
        lax.all_gather(own_head, "dp", axis=0, tiled=True),
    )
    pre1 = jnp.dot(obs, first, preferred_element_type=jnp.float32)
    hidden1 = jax.nn.silu(pre1).astype(jnp.bfloat16)
    columns = hidden1
    pre2 = jnp.dot(
        columns,
        lax.all_gather(own_middle, "dp", axis=0, tiled=True),
        preferred_element_type=jnp.float32,
    )
    hidden2 = jax.nn.silu(pre2).astype(jnp.bfloat16)
    squash = jnp.tanh(jnp.dot(hidden2, head, preferred_element_type=jnp.float32) / CAP)
    logits = CAP * squash
    logp = logits - jnp.log(jnp.sum(jnp.exp(logits), axis=1, keepdims=True))
    onehot = (chosen[:, None] == lax.broadcasted_iota(jnp.int32, logits.shape, 1)).astype(
        jnp.float32
    )
    taken = jnp.sum(logp * onehot, axis=1)
    fitness = lax.psum(jnp.sum(gains * taken) / batch, "dp")
    grad_raw = (
        -(gains / batch)[:, None] * (onehot - jnp.exp(logp)) * (1.0 - squash * squash)
    ).astype(jnp.bfloat16)
    head_term = contract_rows(hidden2, grad_raw)
    grad_pre2 = (contract_cols(grad_raw, head) * silu_slope(pre2)).astype(jnp.bfloat16)
    columns = hidden1
    grad_middle = lax.psum_scatter(
        contract_rows(columns, grad_pre2).astype(jnp.bfloat16),
        "dp",
        scatter_dimension=0,
        tiled=True,
    ).astype(jnp.float32)
    member = lax.axis_index("pop")
    members = lax.axis_size("pop")
    rate = jnp.exp(lax.dynamic_index_in_dim(log_rate, member, keepdims=False))
    new_middle = (own_middle.astype(jnp.float32) - rate * grad_middle).astype(jnp.bfloat16)
    back = contract_cols(grad_pre2, lax.all_gather(own_middle, "dp", axis=0, tiled=True))
    grad_pre1 = (back * silu_slope(pre1)).astype(jnp.bfloat16)
    input_term = contract_rows(obs, grad_pre1)
    grad_first, grad_head = (
        lax.psum_scatter(
            input_term.astype(jnp.bfloat16), "dp", scatter_dimension=0, tiled=True
        ).astype(jnp.float32),
        lax.psum_scatter(
            head_term.astype(jnp.bfloat16), "dp", scatter_dimension=0, tiled=True
        ).astype(jnp.float32),
    )
    new_first = (own_first.astype(jnp.float32) - rate * grad_first).astype(jnp.bfloat16)
    new_head = (own_head.astype(jnp.float32) - rate * grad_head).astype(jnp.bfloat16)
    moved_first, moved_middle, moved_head = shifted((new_first, new_middle, new_head), "pop", 1)
    flag = lax.dynamic_index_in_dim(copy_from, member, keepdims=False) == 1
    out_first = jnp.where(flag, moved_first, new_first)
    out_middle = jnp.where(flag, moved_middle, new_middle)
    out_head = jnp.where(flag, moved_head, new_head)
    source = jnp.where(flag, (member + members - 1) % members, member)
    pick = lax.dynamic_index_in_dim(perturb, member, keepdims=False)
    offset = jnp.where(pick == 0, -0.2, jnp.where(pick == 1, 0.0, 0.2)).astype(jnp.float32)
    next_rate = lax.dynamic_index_in_dim(log_rate, source, keepdims=False) + offset
    return (
        out_first[None],
        out_middle[None],
        out_head[None],
        next_rate.reshape(1),
        fitness.reshape(1),
    )


def solution(mesh):
    in_specs = (
        P("pop", "dp", None),
        P("pop", "dp"),
        P("pop", "dp"),
        P("pop", "dp", None),
        P("pop", "dp", None),
        P("pop", "dp", None),
        P(),
        P(),
        P(),
    )
    out_specs = (
        P("pop", "dp", None),
        P("pop", "dp", None),
        P("pop", "dp", None),
        P("pop"),
        P("pop"),
    )

    def step(*arrays):
        observations, w_middle = arrays[0], arrays[4]
        small = observations.shape[1] // 2 <= w_middle.shape[2] and mesh.shape["dp"] % 4 == 0
        body = hub_step if small else local
        step = jax.shard_map(body, mesh=mesh, in_specs=in_specs, out_specs=out_specs, check_vma=False)
        return step(*arrays)

    return step
```

```python
import jax
import jax.numpy as jnp
from jax import lax
from jax.experimental import pallas as pl
from jax.experimental.pallas import tpu as pltpu
from jax.sharding import PartitionSpec as P

CAP = 2.0
PARTS = (2, 2)
GROUPS = 2


def silu_slope(pre):
    sig = jax.nn.sigmoid(pre)
    return sig * (1.0 + pre * (1.0 - sig))


def contract_rows(left, right):
    return lax.dot_general(
        left, right, (((0,), (0,)), ((), ())), preferred_element_type=jnp.float32
    )


def contract_cols(left, right):
    return lax.dot_general(
        left, right, (((1,), (1,)), ((), ())), preferred_element_type=jnp.float32
    )


def sigmoid(v):
    return 0.5 + 0.5 * jnp.tanh(0.5 * v)


def dot(left, right, dims=((1,), (0,))):
    return lax.dot_general(left, right, (dims, ((), ())), preferred_element_type=jnp.float32)


def params(mib, *semantics):
    return pltpu.CompilerParams(dimension_semantics=semantics or None, vmem_limit_bytes=mib << 20)


def hbm(array):
    return pltpu.with_memory_space_constraint(array, pltpu.HBM)


def whole(array):
    return pl.BlockSpec(array.shape, lambda *_: (0,) * array.ndim)


def cost(flops, moved):
    return pl.CostEstimate(flops=int(flops), bytes_accessed=int(moved), transcendentals=0)


def pack(obs, first, head, gains, chosen, slab, pad_acts):
    rows, features = obs.shape
    each, width = first.shape
    devices = width // slab
    acts = head.shape[1]
    mids = devices * each
    per = rows // features
    at = rows + mids + pad_acts
    total = at + -(-4 * per // 16) * 16

    def kernel(obs_ref, first_ref, head_ref, gains_ref, chosen_ref, out_ref):
        out_ref[:rows, :] = obs_ref[...]
        for b in range(devices):
            out_ref[rows + b * each : rows + (b + 1) * each, :] = first_ref[:, b * slab : (b + 1) * slab]
        block = head_ref[...].astype(jnp.float32)
        block = jnp.concatenate([block, jnp.zeros((slab, 128 - acts), jnp.float32)], axis=1)
        out_ref[rows + mids : at, :] = block.T[:pad_acts].astype(jnp.bfloat16)
        out_ref[at:, :] = jnp.zeros((total - at, features), jnp.bfloat16)
        value = gains_ref[...]
        parts = []
        for _ in range(3):
            parts.append(value.astype(jnp.bfloat16))
            value = value - parts[-1].astype(jnp.float32)
        parts.append(chosen_ref[...].astype(jnp.float32).astype(jnp.bfloat16))
        for t, part in enumerate(parts):
            for r in range(per):
                row = at + t * per + r
                out_ref[row : row + 1, :] = part[:, r * features : (r + 1) * features]

    arrays = (obs, first, head, gains, chosen)
    return pl.pallas_call(
        kernel,
        name="pack",
        grid=(1,),
        in_specs=[whole(v) for v in arrays],
        out_specs=pl.BlockSpec((total, features), lambda i: (0, 0)),
        out_shape=pltpu.HBM((total, features), jnp.bfloat16),
        cost_estimate=cost(1 << 24, 1 << 20),
        compiler_params=params(6, "arbitrary"),
    )(*map(hbm, arrays))


def first_layer(order, scalars, pieces, theirs, rows, slab, near_blocks, pad_acts):
    count = len(pieces)
    devices = 2 * count
    features = pieces[0].shape[1]
    each = features // devices
    mids = devices * each
    width = devices * slab
    total = count * rows
    near_all = 2 * near_blocks

    def near_at(i):
        return (i // count) * near_blocks + jnp.minimum(i % count, near_blocks - 1)

    def kernel(order_ref, scalar_ref, *refs):
        live = scalar_ref[2] == 1
        piece_refs, theirs_ref = refs[:count], refs[count]
        h1_ref, h1t_ref, slope_ref, obst_ref, head_ref, cols = refs[count + 1 :]
        i = pl.program_id(0)

        def small(k, start, size):
            if k < count:
                return piece_refs[k][pl.ds(rows + start, size), :]
            return theirs_ref[k - count, pl.ds(start, size), :]

        @pl.when(live & (i == 0))
        def _():
            for k in range(devices):
                at = pl.multiple_of(order_ref[k] * each, each)
                lanes = pl.multiple_of(order_ref[k] * slab, slab)
                head_ref[:, pl.ds(lanes, slab)] = small(k, mids, pad_acts)
                for b in range(devices):
                    source = pl.multiple_of(order_ref[b] * each, each)
                    cols[b, pl.ds(at, each), :] = small(k, source, each)
            for p in range(count):
                block = piece_refs[p][:rows, :].astype(jnp.float32)
                obst_ref[:, p * rows : (p + 1) * rows] = block.T.astype(jnp.bfloat16)

        close = i % count < near_blocks

        @pl.when(live & close)
        def _():
            weights = cols[i]
            for p in range(count):
                at = slice(p * rows, (p + 1) * rows)
                obs = piece_refs[p][:rows, :]
                pre = dot(obs, weights)
                sig = sigmoid(pre)
                h1_ref[at, :] = (pre * sig).astype(jnp.bfloat16)
                slope_ref[at, :] = (sig * (1.0 + pre * (1.0 - sig))).astype(jnp.bfloat16)
                pre_t = dot(weights, obs, ((0,), (1,)))
                h1t_ref[:, at] = (pre_t * sigmoid(pre_t)).astype(jnp.bfloat16)

        @pl.when(live & jnp.logical_not(close))
        def _():
            weights = cols[i]
            for p in range(count):
                pre = dot(piece_refs[p][:rows, :], weights)
                h1_ref[p * rows : (p + 1) * rows, :] = (pre * sigmoid(pre)).astype(jnp.bfloat16)

    shape = lambda *s: jax.ShapeDtypeStruct(s, jnp.bfloat16)
    return pl.pallas_call(
        kernel,
        name="first_layer",
        grid_spec=pltpu.PrefetchScalarGridSpec(
            num_scalar_prefetch=2,
            grid=(devices,),
            in_specs=[whole(p) for p in pieces] + [whole(theirs)],
            out_specs=[
                pl.BlockSpec((total, slab), lambda i, *_: (0, i)),
                pl.BlockSpec((slab, total), lambda i, *_: (near_at(i), 0)),
                pl.BlockSpec((total, slab), lambda i, *_: (0, near_at(i))),
                pl.BlockSpec((features, total), lambda i, *_: (0, 0)),
                pl.BlockSpec((pad_acts, width), lambda i, *_: (0, 0)),
            ],
            scratch_shapes=[pltpu.VMEM((devices, features, slab), jnp.bfloat16)],
        ),
        out_shape=[
            shape(total, width),
            shape(near_all * slab, total),
            pltpu.HBM((total, near_all * slab), jnp.bfloat16),
            pltpu.HBM((features, total), jnp.bfloat16),
            shape(pad_acts, width),
        ],
        cost_estimate=cost(2 * total * features * width * 2, 30 << 20),
        compiler_params=params(20, "arbitrary"),
    )(order, scalars, *map(hbm, pieces), theirs)


def second_layer(scalars, hidden1, own, pieces, theirs, head, logits, hidden2, start, inner, cut):
    total, width = hidden1.shape
    slab = own.shape[0]
    pad_acts = head.shape[0]
    tile = min(512, total)
    first = logits is None
    sub = 256
    q = start // cut

    def kernel(scalar_ref, h1_ref, own_ref, *refs):
        live = scalar_ref[2] == 1
        piece_refs = refs[: len(pieces)]
        theirs_ref, head_ref = refs[len(pieces) : len(pieces) + 2]
        rest = refs[len(pieces) + 2 :]
        logits_in = None if first else rest[0]
        h2_ref, slope_ref, logits_ref, weights = rest[0 if first else 2 :]

        @pl.when(live & (pl.program_id(0) == 0))
        def _():
            weights[:slab] = own_ref[...]
            for k, piece in enumerate(piece_refs):
                weights[(k + 1) * slab : (k + 2) * slab] = piece[...]
            weights[(len(pieces) + 1) * slab :] = theirs_ref[...]

        @pl.when(live)
        def _():
            for r in range(0, tile, sub):
                pre = dot(h1_ref[r : r + sub, :], weights[...])
                sig = sigmoid(pre)
                hidden = (pre * sig).astype(jnp.bfloat16)
                h2_ref[r : r + sub, :] = hidden
                slope_ref[r : r + sub, :] = (sig * (1.0 + pre * (1.0 - sig))).astype(jnp.bfloat16)
                part = dot(hidden, head_ref[...], ((1,), (1,)))
                logits_ref[r : r + sub, :] = part if first else part + logits_in[r : r + sub, :]

    row = lambda size: pl.BlockSpec((tile, size), lambda i: (i, 0))
    return pl.pallas_call(
        kernel,
        name="second_layer",
        grid=(total // tile,),
        in_specs=[pl.BlockSpec(memory_space=pltpu.SMEM), row(width), pl.BlockSpec((slab, cut), lambda i: (0, q))]
        + [pl.BlockSpec((slab, cut), lambda i: (0, inner))] * len(pieces)
        + [pl.BlockSpec((theirs.shape[0], cut), lambda i: (0, inner)), pl.BlockSpec((pad_acts, cut), lambda i: (0, q))]
        + ([] if first else [row(pad_acts), pl.BlockSpec(memory_space=pltpu.HBM)]),
        out_specs=[pl.BlockSpec((tile, cut), lambda i: (i, q)), row(cut), row(pad_acts)],
        out_shape=[
            pltpu.HBM((total, width), jnp.bfloat16),
            jax.ShapeDtypeStruct((total, cut), jnp.bfloat16),
            jax.ShapeDtypeStruct((total, pad_acts), jnp.float32),
        ],
        scratch_shapes=[pltpu.VMEM((width, cut), jnp.bfloat16)],
        input_output_aliases={} if first else {len(pieces) + 6: 0},
        cost_estimate=cost(2 * total * width * cut, 16 << 20),
        compiler_params=params(12 + (8 * width * cut >> 20), "arbitrary"),
    )(scalars, hidden1, hbm(own), *pieces, theirs, head, *([] if first else [logits, hbm(hidden2)]))


def policy(logits_raw, pieces, at, acts, batch):
    total, pad_acts = logits_raw.shape
    count = len(pieces)
    features = pieces[0].shape[1]
    per = total // count // features
    size = pieces[0].shape[0] - at

    def kernel(raw_ref, *refs):
        label_refs = refs[:count]
        graw_ref, graw_t_ref, score_ref = refs[count:]
        raw = raw_ref[...].T
        blocks = [ref[...].astype(jnp.float32) for ref in label_refs]
        part = lambda t: jnp.concatenate(
            [block[t * per + r : t * per + r + 1, :] for block in blocks for r in range(per)], axis=1
        )
        gains, chosen = part(0) + part(1) + part(2), part(3).astype(jnp.int32)
        at = lax.broadcasted_iota(jnp.int32, raw.shape, 0)
        live = at < acts
        squash = jnp.tanh(raw / CAP)
        logits = CAP * squash
        mass = jnp.sum(jnp.where(live, jnp.exp(logits), 0.0), axis=0, keepdims=True)
        logp = logits - jnp.log(mass)
        onehot = at == chosen
        taken = jnp.sum(jnp.where(onehot, logp, 0.0), axis=0, keepdims=True)
        score_ref[...] = jnp.sum(gains * taken, axis=1, keepdims=True) / batch
        grad = -(gains / batch) * (onehot.astype(jnp.float32) - jnp.exp(logp)) * (1.0 - squash * squash)
        grad = jnp.where(live, grad, 0.0)
        graw_t_ref[...] = grad.astype(jnp.bfloat16)
        graw_ref[...] = grad.T.astype(jnp.bfloat16)

    return pl.pallas_call(
        kernel,
        name="policy",
        grid=(1,),
        in_specs=[whole(logits_raw)] + [pl.BlockSpec((size, features), lambda i: (at // size, 0))] * count,
        out_specs=[
            pl.BlockSpec((total, pad_acts), lambda i: (0, 0)),
            pl.BlockSpec((pad_acts, total), lambda i: (0, 0)),
            pl.BlockSpec((1, 1), lambda i: (0, 0)),
        ],
        out_shape=[
            jax.ShapeDtypeStruct((total, pad_acts), jnp.bfloat16),
            jax.ShapeDtypeStruct((pad_acts, total), jnp.bfloat16),
            jax.ShapeDtypeStruct((1, 1), jnp.float32),
        ],
        cost_estimate=cost(1 << 28, 2 << 20),
        compiler_params=params(10, "arbitrary"),
    )(logits_raw, *map(hbm, pieces))


def middle_grad(scalars, graw, head, slopes, hidden1_t, start, cut):
    total, pad_acts = graw.shape
    near_rows = hidden1_t.shape[0]
    kept = near_rows // 2
    tile = min(256, kept)
    steps = near_rows // tile
    parts = len(slopes)
    span = parts * cut

    def kernel(scalar_ref, graw_ref, head_ref, *refs):
        live = scalar_ref[2] == 1
        slope_refs = refs[:parts]
        h1t_ref, g2_ref, keep_ref, give_ref = refs[parts:]
        i = pl.program_id(0)

        @pl.when(live & (i == 0))
        def _():
            for p in range(parts):
                lanes = slice(p * cut, (p + 1) * cut)
                for r in range(0, total, 256):
                    g2 = dot(graw_ref[r : r + 256, :], head_ref[:, lanes]) * slope_refs[p][r : r + 256, :].astype(jnp.float32)
                    g2_ref[r : r + 256, lanes] = g2.astype(jnp.bfloat16)

        @pl.when(live & (i < steps // 2))
        def _():
            give_ref[...] = dot(h1t_ref[...], g2_ref[...]).astype(jnp.bfloat16)

        @pl.when(live & (i >= steps // 2))
        def _():
            keep_ref[...] = dot(h1t_ref[...], g2_ref[...])

    turn = lambda i: (i + steps // 2) % steps
    return pl.pallas_call(
        kernel,
        name="middle_grad",
        grid=(steps,),
        in_specs=[pl.BlockSpec(memory_space=pltpu.SMEM), whole(graw), pl.BlockSpec((pad_acts, span), lambda i: (0, start // span))]
        + [whole(v) for v in slopes]
        + [pl.BlockSpec((tile, total), lambda i: (turn(i), 0))],
        out_specs=[
            pl.BlockSpec((total, span), lambda i: (0, 0)),
            pl.BlockSpec((tile, span), lambda i: (jnp.maximum(i - steps // 2, 0), 0)),
            pl.BlockSpec((tile, span), lambda i: (jnp.minimum(i, steps // 2 - 1), 0)),
        ],
        out_shape=[
            pltpu.HBM((total, span), jnp.bfloat16),
            jax.ShapeDtypeStruct((kept, span), jnp.float32),
            pltpu.HBM((kept, span), jnp.bfloat16),
        ],
        cost_estimate=cost(2 * total * near_rows * span, 16 << 20),
        compiler_params=params(24, "arbitrary"),
    )(scalars, graw, head, *slopes, hidden1_t)


def head_grad(scalars, graw_t, hidden2):
    pad_acts, total = graw_t.shape
    side = hidden2.shape[1] // 2
    block = min(512, side)

    def kernel(scalar_ref, graw_t_ref, h2_ref, out_ref):
        out_ref[...] = dot(graw_t_ref[...], h2_ref[...])

    return pl.pallas_call(
        kernel,
        name="head_grad",
        grid_spec=pltpu.PrefetchScalarGridSpec(
            num_scalar_prefetch=1,
            grid=(side // block,),
            in_specs=[
                pl.BlockSpec((pad_acts, total), lambda i, _: (0, 0)),
                pl.BlockSpec((total, block), lambda i, s: (0, s[1] * (side // block) + i)),
            ],
            out_specs=pl.BlockSpec((pad_acts, block), lambda i, _: (0, i)),
        ),
        out_shape=jax.ShapeDtypeStruct((pad_acts, side), jnp.float32),
        cost_estimate=cost(2 * total * side * 256, 6 << 20),
        compiler_params=params(10, "arbitrary"),
    )(scalars, graw_t, hbm(hidden2))


def middle_update(rate, keep, got, own, near_pieces, group, span, cut):
    slab = own.shape[0]
    per = span // cut
    blocks = 1 + len(near_pieces[0])
    flat = [p for chunk in near_pieces for p in chunk]

    def kernel(rate_ref, keep_ref, got_ref, own_ref, *refs):
        flat_refs, out_refs = refs[: len(flat)], refs[len(flat) :]
        rate = rate_ref[0:1, 0:1]
        for s in reversed(range(blocks)):
            for p in range(per):
                lanes, at = slice(p * cut, (p + 1) * cut), slice(s * slab, (s + 1) * slab)
                weight = own_ref[:, lanes] if s == 0 else flat_refs[p * (blocks - 1) + s - 1][...]
                total = keep_ref[at, lanes] + got_ref[at, lanes].astype(jnp.float32)
                out_refs[s][:, lanes] = (weight.astype(jnp.float32) - rate * total).astype(jnp.bfloat16)

    return pl.pallas_call(
        kernel,
        name="middle_update",
        grid=(1,),
        in_specs=[whole(rate), whole(keep), whole(got)]
        + [pl.BlockSpec((slab, span), lambda i: (0, group))]
        + [whole(p) for p in flat],
        out_specs=[pl.BlockSpec((slab, span), lambda i: (0, 0))] * blocks,
        out_shape=[pltpu.HBM((slab, span), jnp.bfloat16)] * blocks,
        cost_estimate=cost(1 << 27, 4 << 20),
        compiler_params=params(16, "arbitrary"),
    )(rate, keep, got, hbm(own), *flat)


def gather_small(scalars, order, keep, got, side, score, first_rows, slab, half):
    count = 2 * half
    devices = 2 * count
    mids = devices * first_rows
    pad_acts = side.shape[0]
    acts_at = mids + pad_acts

    def kernel(scalar_ref, order_ref, keep_ref, got_ref, side_ref, score_ref, mine_ref, sent_ref):
        core = scalar_ref[0]
        for target, which in ((sent_ref, 1 - core), (mine_ref, core)):
            for j in range(half):
                base = pl.multiple_of(j * 2 * first_rows + which * first_rows, first_rows)
                for k in range(devices):
                    source = got_ref if (k // half) % 2 else keep_ref
                    lanes = ((k // count) * half + k % half) * slab
                    at = pl.multiple_of(order_ref[k] * first_rows, first_rows)
                    target[j, pl.ds(at, first_rows), :] = source[pl.ds(base, first_rows), lanes : lanes + slab]
                cols = pl.multiple_of((j * 2 + which) * slab, slab)
                target[j, mids:acts_at, :] = side_ref[:, pl.ds(cols, slab)].astype(jnp.bfloat16)
        value = jnp.broadcast_to(score_ref[...], (1, slab))
        for part in range(3):
            piece = value.astype(jnp.bfloat16)
            sent_ref[0, acts_at - 3 + part : acts_at - 2 + part, :] = piece
            value = value - piece.astype(jnp.float32)

    shape = jax.ShapeDtypeStruct((half, acts_at, slab), jnp.bfloat16)
    smem = pl.BlockSpec(memory_space=pltpu.SMEM)
    arrays = [keep, got, side, score]
    return pl.pallas_call(
        kernel,
        name="gather_small",
        grid=(1,),
        in_specs=[smem, smem] + [whole(v) for v in arrays],
        out_specs=[whole(shape)] * 2,
        out_shape=[shape, pltpu.HBM(shape.shape, shape.dtype)],
        cost_estimate=cost(1 << 26, 2 << 20),
        compiler_params=params(8, "arbitrary"),
    )(scalars, order, *arrays)


def small_update(scalars, rate, mine, got, weights, score, at_row):
    half, rows, slab = mine.shape

    def kernel(scalar_ref, rate_ref, mine_ref, got_ref, *refs):
        weight_refs = refs[:half]
        score_ref, fitness_ref = refs[half], refs[half + 1]
        out_refs = refs[half + 2 :]
        rate, high = rate_ref[0:1, 0:1], scalar_ref[1]
        fitness = jnp.broadcast_to(score_ref[...], (1, slab))
        for part in range(3):
            fitness = fitness + got_ref[0, rows - 3 + part : rows - 2 + part, :].astype(jnp.float32)
        fitness_ref[...] = fitness[:, :1]
        for s in range(half):
            at = jnp.where(high == 1, s, half - 1 - s)
            total = mine_ref[at].astype(jnp.float32) + got_ref[at].astype(jnp.float32)
            out_refs[s][...] = (weight_refs[s][at_row : at_row + rows, :].astype(jnp.float32) - rate * total).astype(jnp.bfloat16)
            value = fitness
            for part in range(3):
                piece = value.astype(jnp.bfloat16)
                out_refs[s][rows - 3 + part : rows - 2 + part, :] = piece
                value = value - piece.astype(jnp.float32)

    smem = pl.BlockSpec(memory_space=pltpu.SMEM)
    return pl.pallas_call(
        kernel,
        name="small_update",
        grid=(1,),
        in_specs=[smem] + [whole(v) for v in (rate, mine, got, *weights, score)],
        out_specs=[pl.BlockSpec((1, 1), lambda i: (0, 0))] + [pl.BlockSpec((rows, slab), lambda i: (0, 0))] * half,
        out_shape=[jax.ShapeDtypeStruct((1, 1), jnp.float32)] + [pltpu.HBM((rows, slab), jnp.bfloat16)] * half,
        cost_estimate=cost(1 << 26, 2 << 20),
        compiler_params=params(8, "arbitrary"),
    )(scalars, rate, mine, got, *map(hbm, weights), score)


def input_grad(scalars, grads, own, near_pieces, theirs, slope, obs_t):
    total = grads[0].shape[0]
    slab, width = own.shape
    near_rows = slope.shape[1]
    kept = near_rows // 2
    features = obs_t.shape[0]
    groups = len(grads)
    chunks = len(theirs)
    side = features // 2
    tile = min(512, total)
    cuts = [v.shape[1] for v in theirs]
    starts = [sum(cuts[:q]) for q in range(chunks)]
    flat = [p for chunk in near_pieces for p in chunk]
    per = len(flat) // chunks

    def kernel(scalar_ref, *refs):
        g_refs, refs = refs[:groups], refs[groups:]
        own_ref, refs = refs[0], refs[1:]
        flat_refs, refs = refs[: len(flat)], refs[len(flat) :]
        theirs_refs, refs = refs[:chunks], refs[chunks:]
        slope_ref, obst_ref, keep_ref, give_ref, weights, total_ref = refs
        i = pl.program_id(0)
        live = scalar_ref[2] == 1

        @pl.when(live & (i == 0))
        def _():
            weights[:slab] = own_ref[...]
            for q in range(chunks):
                lanes = slice(starts[q], starts[q] + cuts[q])
                for k in range(per):
                    weights[(k + 1) * slab : (k + 2) * slab, lanes] = flat_refs[q * per + k][...]
                weights[kept:, lanes] = theirs_refs[q][...]
            total_ref[...] = jnp.zeros_like(total_ref)

        @pl.when(live)
        def _():
            g2 = jnp.concatenate([g[...] for g in g_refs], axis=1)
            back = dot(g2, weights[...], ((1,), (1,)))
            grad = (back * slope_ref[...].astype(jnp.float32)).astype(jnp.bfloat16)
            total_ref[...] += dot(obst_ref[...], grad)

        @pl.when(live & (i == pl.num_programs(0) - 1))
        def _():
            high = scalar_ref[1]
            keep_ref[...] = total_ref[pl.ds(pl.multiple_of(high * side, side), side), :].astype(jnp.bfloat16)
            give_ref[...] = total_ref[pl.ds(pl.multiple_of((1 - high) * side, side), side), :].astype(jnp.bfloat16)

    return pl.pallas_call(
        kernel,
        name="input_grad",
        grid=(total // tile,),
        in_specs=[pl.BlockSpec(memory_space=pltpu.SMEM)]
        + [pl.BlockSpec((tile, g.shape[1]), lambda i: (i, 0)) for g in grads]
        + [whole(own)]
        + [whole(p) for p in flat]
        + [pl.BlockSpec((kept, cut), lambda i: (0, 0)) for cut in cuts]
        + [pl.BlockSpec((tile, near_rows), lambda i: (i, 0)), pl.BlockSpec((features, tile), lambda i: (0, i))],
        out_specs=[pl.BlockSpec((side, near_rows), lambda i: (0, 0))] * 2,
        out_shape=[
            jax.ShapeDtypeStruct((side, near_rows), jnp.bfloat16),
            pltpu.HBM((side, near_rows), jnp.bfloat16),
        ],
        scratch_shapes=[
            pltpu.VMEM((near_rows, width), jnp.bfloat16),
            pltpu.VMEM((features, near_rows), jnp.float32),
        ],
        cost_estimate=cost(2 * total * near_rows * width, 20 << 20),
        compiler_params=params(34, "arbitrary"),
    )(scalars, *map(hbm, grads), hbm(own), *map(hbm, flat), *map(hbm, theirs), hbm(slope), hbm(obs_t))


def settings(numbers, log_rate, copy_from, perturb, devices):
    members = log_rate.shape[0]

    def kernel(numbers_ref, log_rate_ref, copy_ref, perturb_ref, order_ref, scalars_ref, rate_ref, flag_ref, next_ref):
        for k in range(devices):
            order_ref[k] = numbers_ref[k]
        for k in range(3):
            scalars_ref[k] = numbers_ref[devices + k]
        member = numbers_ref[devices + 3]
        rate_ref[...] = jnp.exp(jnp.full(rate_ref.shape, log_rate_ref[member], jnp.float32))
        taken = copy_ref[member] == 1
        flag_ref[0] = taken.astype(jnp.int32)
        source = jnp.where(taken, lax.rem(member + members - 1, members), member)
        pick = perturb_ref[member]
        offset = jnp.where(pick == 0, -0.2, jnp.where(pick == 1, 0.0, 0.2)).astype(jnp.float32)
        next_ref[...] = jnp.full(next_ref.shape, log_rate_ref[source] + offset, jnp.float32)

    smem = pl.BlockSpec(memory_space=pltpu.SMEM)
    vmem = pl.BlockSpec(memory_space=pltpu.VMEM)
    ints = lambda n: jax.ShapeDtypeStruct((n,), jnp.int32)
    return pl.pallas_call(
        kernel,
        name="settings",
        in_specs=[smem] * 4,
        out_specs=[smem, smem, vmem, smem, vmem],
        out_shape=[
            ints(devices),
            ints(3),
            jax.ShapeDtypeStruct((8, 128), jnp.float32),
            ints(1),
            jax.ShapeDtypeStruct((1, 1), jnp.float32),
        ],
        cost_estimate=cost(1 << 10, 1 << 10),
        compiler_params=params(4),
    )(numbers, log_rate, copy_from, perturb)


def hub_body(observations, returns, actions, w_input, w_middle, w_head, log_rate, copy_from, perturb):
    obs = observations[0]
    own_first, own_middle, own_head = w_input[0], w_middle[0], w_head[0]
    devices = lax.axis_size("dp")
    half = devices // 4
    count = 2 * half
    rows, _ = obs.shape
    first_rows, width = own_first.shape
    slab = own_middle.shape[0]
    acts = own_head.shape[1]
    pad_acts = -(-(acts + 3) // 32) * 32
    batch = rows * devices
    mids = devices * first_rows
    cuts = [width // part for part in PARTS]
    starts = [sum(cuts[:q]) for q in range(len(cuts))]
    cut = min(cuts)
    place = lax.axis_index("dp")
    core = place % 2
    chip = place // 2
    high = (chip >= half).astype(jnp.int32)
    member = lax.axis_index("pop")
    members = lax.axis_size("pop")
    ring = [(i, (i + 1) % members) for i in range(members)]

    def side(step, upper):
        return half + step if upper else half - 1 - step

    def route(step, crossing, back=False):
        pairs = []
        for upper in (False, True):
            hub = side(0, upper != crossing)
            end = side(step, upper)
            pairs += [(2 * end + c, 2 * hub + c) for c in range(2)]
        return [(b, a) for a, b in pairs] if back else pairs

    def near(value, step):
        return lax.ppermute(value, "dp", route(step, False))

    def far(value, step):
        return lax.ppermute(value, "dp", route(step, True))

    def outward(value, step):
        return lax.ppermute(value, "dp", route(step, False, True))

    def partner(value):
        return lax.ppermute(value, "dp", [(i, i ^ 1) for i in range(devices)])

    def shifted(value):
        return lax.ppermute(value, "pop", ring)

    slots = jnp.arange(devices, dtype=jnp.int32)
    upper = high ^ ((slots // half) % 2)
    order = 2 * jnp.where(upper == 1, half + slots % half, half - 1 - slots % half) + (core ^ (slots // count))

    hub = ((chip == half) | (chip == half - 1)).astype(jnp.int32)
    numbers = jnp.concatenate([order, jnp.stack([core, high, hub, member])]).astype(jnp.int32)
    order, scalars, rate, flag, next_rate = settings(numbers, log_rate, copy_from, perturb, devices)

    def column(value):
        out = []
        for s in range(1, half):
            out.append(near(value, s))
        for s in range(half):
            out.append(far(value, s))
        return out

    labels_at = rows + mids + pad_acts
    packed = pack(obs, own_first, own_head, returns, actions, slab, pad_acts)
    pieces = [packed] + column(packed)
    columns = [own_middle[:, start : start + cut] for start, cut in zip(starts, cuts)]
    middle_pieces = [column(columns[q]) for q in range(len(cuts))]
    theirs_small = partner(jnp.stack([p[rows:labels_at] for p in pieces]))
    hidden1, near_t, slope1, obs_t, head = first_layer(order, scalars, pieces, theirs_small, rows, slab, half, pad_acts)

    logits = None
    hidden2, slope2, theirs = None, [], []
    for q in range(len(cuts)):
        mine = jnp.concatenate([columns[q]] + middle_pieces[q], axis=0)
        theirs.append(partner(mine))
        for inner in range(cuts[q] // cut):
            start = starts[q] + inner * cut
            hidden2, slope, logits = second_layer(
                scalars, hidden1, own_middle, middle_pieces[q], theirs[q], head, logits, hidden2, start, inner, cut
            )
            slope2.append(slope)

    grad_raw, grad_raw_t, score = policy(logits, pieces, labels_at, acts, batch)

    distance = jnp.where(high == 1, chip - half, half - 1 - chip)

    def home(blocks):
        out = blocks[0]
        for s in range(1, half):
            moved = outward(blocks[s], s)
            out = jnp.where(distance == s, moved, out)
        return out

    flag = flag[0] == 1

    near_w = [m[: half - 1] for m in middle_pieces]
    span = width // GROUPS
    out_middle, grads = [], []
    for g in range(GROUPS):
        which = [q for q in range(len(cuts)) if starts[q] // span == g]
        parts = range(g * span // cut, (g + 1) * span // cut)
        g2, keep, give = middle_grad(scalars, grad_raw, head, [slope2[p] for p in parts], near_t, g * span, cut)
        got = partner(give)
        new = middle_update(rate, keep, got, own_middle, [near_w[q] for q in which], g, span, cuts[which[0]])
        new = home(new)
        moved = shifted(new)
        out_middle.append(jnp.where(flag, moved, new))
        grads.append(g2)
    out_middle = jnp.concatenate(out_middle, axis=1)

    keep, give = input_grad(scalars, grads, own_middle, near_w, theirs, slope1, obs_t)
    got = far(give, 0)
    head_term = head_grad(scalars, grad_raw_t, hidden2)
    mine, sent = gather_small(scalars, order, keep, got, head_term, score, first_rows, slab, half)
    got = partner(sent)
    fitness, *new_small = small_update(scalars, rate, mine, got, pieces[:half], score, rows)
    new_small = home(new_small)
    fitness = jnp.where(
        distance == 0, fitness, jnp.sum(new_small[-3:, :1].astype(jnp.float32), axis=0, keepdims=True)
    )
    moved = shifted(new_small)
    out_small = jnp.where(flag, moved, new_small)
    out_first = out_small[:mids].reshape(devices, first_rows, slab).swapaxes(0, 1).reshape(first_rows, width)
    out_head = out_small[mids : mids + acts].T

    return (
        out_first[None],
        out_middle[None],
        out_head[None],
        next_rate.reshape(1),
        fitness.reshape(1),
    )


def hub_step(*arrays):
    return hub_body(*arrays)


def shifted(block, axis, distance):
    devices = range(lax.axis_size(axis))
    route = [((i - distance) % len(devices), i) for i in devices]
    return lax.ppermute(block, axis, route)


def local(observations, returns, actions, w_input, w_middle, w_head, log_rate, copy_from, perturb):
    obs = observations[0]
    gains = returns[0]
    chosen = actions[0]
    own_first = w_input[0]
    own_middle = w_middle[0]
    own_head = w_head[0]
    rows = obs.shape[0]
    batch = rows * lax.axis_size("dp")
    first, head = (
        lax.all_gather(own_first, "dp", axis=0, tiled=True),
        lax.all_gather(own_head, "dp", axis=0, tiled=True),
    )
    pre1 = jnp.dot(obs, first, preferred_element_type=jnp.float32)
    hidden1 = jax.nn.silu(pre1).astype(jnp.bfloat16)
    columns = hidden1
    pre2 = jnp.dot(
        columns,
        lax.all_gather(own_middle, "dp", axis=0, tiled=True),
        preferred_element_type=jnp.float32,
    )
    hidden2 = jax.nn.silu(pre2).astype(jnp.bfloat16)
    squash = jnp.tanh(jnp.dot(hidden2, head, preferred_element_type=jnp.float32) / CAP)
    logits = CAP * squash
    logp = logits - jnp.log(jnp.sum(jnp.exp(logits), axis=1, keepdims=True))
    onehot = (chosen[:, None] == lax.broadcasted_iota(jnp.int32, logits.shape, 1)).astype(
        jnp.float32
    )
    taken = jnp.sum(logp * onehot, axis=1)
    fitness = lax.psum(jnp.sum(gains * taken) / batch, "dp")
    grad_raw = (
        -(gains / batch)[:, None] * (onehot - jnp.exp(logp)) * (1.0 - squash * squash)
    ).astype(jnp.bfloat16)
    head_term = contract_rows(hidden2, grad_raw)
    grad_pre2 = (contract_cols(grad_raw, head) * silu_slope(pre2)).astype(jnp.bfloat16)
    columns = hidden1
    grad_middle = lax.psum_scatter(
        contract_rows(columns, grad_pre2).astype(jnp.bfloat16),
        "dp",
        scatter_dimension=0,
        tiled=True,
    ).astype(jnp.float32)
    member = lax.axis_index("pop")
    members = lax.axis_size("pop")
    rate = jnp.exp(lax.dynamic_index_in_dim(log_rate, member, keepdims=False))
    new_middle = (own_middle.astype(jnp.float32) - rate * grad_middle).astype(jnp.bfloat16)
    back = contract_cols(grad_pre2, lax.all_gather(own_middle, "dp", axis=0, tiled=True))
    grad_pre1 = (back * silu_slope(pre1)).astype(jnp.bfloat16)
    input_term = contract_rows(obs, grad_pre1)
    grad_first, grad_head = (
        lax.psum_scatter(
            input_term.astype(jnp.bfloat16), "dp", scatter_dimension=0, tiled=True
        ).astype(jnp.float32),
        lax.psum_scatter(
            head_term.astype(jnp.bfloat16), "dp", scatter_dimension=0, tiled=True
        ).astype(jnp.float32),
    )
    new_first = (own_first.astype(jnp.float32) - rate * grad_first).astype(jnp.bfloat16)
    new_head = (own_head.astype(jnp.float32) - rate * grad_head).astype(jnp.bfloat16)
    moved_first, moved_middle, moved_head = shifted((new_first, new_middle, new_head), "pop", 1)
    flag = lax.dynamic_index_in_dim(copy_from, member, keepdims=False) == 1
    out_first = jnp.where(flag, moved_first, new_first)
    out_middle = jnp.where(flag, moved_middle, new_middle)
    out_head = jnp.where(flag, moved_head, new_head)
    source = jnp.where(flag, (member + members - 1) % members, member)
    pick = lax.dynamic_index_in_dim(perturb, member, keepdims=False)
    offset = jnp.where(pick == 0, -0.2, jnp.where(pick == 1, 0.0, 0.2)).astype(jnp.float32)
    next_rate = lax.dynamic_index_in_dim(log_rate, source, keepdims=False) + offset
    return (
        out_first[None],
        out_middle[None],
        out_head[None],
        next_rate.reshape(1),
        fitness.reshape(1),
    )


def solution(mesh):
    in_specs = (
        P("pop", "dp", None),
        P("pop", "dp"),
        P("pop", "dp"),
        P("pop", "dp", None),
        P("pop", "dp", None),
        P("pop", "dp", None),
        P(),
        P(),
        P(),
    )
    out_specs = (
        P("pop", "dp", None),
        P("pop", "dp", None),
        P("pop", "dp", None),
        P("pop"),
        P("pop"),
    )

    def step(*arrays):
        observations, w_middle = arrays[0], arrays[4]
        small = observations.shape[1] // 2 <= w_middle.shape[2] and mesh.shape["dp"] % 4 == 0
        small = small and arrays[3].shape[1] * mesh.shape["dp"] == w_middle.shape[2]
        body = hub_step if small else local
        step = jax.shard_map(body, mesh=mesh, in_specs=in_specs, out_specs=out_specs, check_vma=False)
        return step(*arrays)

    return step
```

```python
import jax
import jax.numpy as jnp
from jax import lax
from jax.experimental import pallas as pl
from jax.experimental.pallas import tpu as pltpu
from jax.sharding import PartitionSpec as P

CAP = 2.0
PARTS = (2, 2)
GROUPS = 2


def silu_slope(pre):
    sig = jax.nn.sigmoid(pre)
    return sig * (1.0 + pre * (1.0 - sig))


def contract_rows(left, right):
    return lax.dot_general(
        left, right, (((0,), (0,)), ((), ())), preferred_element_type=jnp.float32
    )


def contract_cols(left, right):
    return lax.dot_general(
        left, right, (((1,), (1,)), ((), ())), preferred_element_type=jnp.float32
    )


def sigmoid(v):
    return 0.5 + 0.5 * jnp.tanh(0.5 * v)


def dot(left, right, dims=((1,), (0,))):
    return lax.dot_general(left, right, (dims, ((), ())), preferred_element_type=jnp.float32)


def params(mib, *semantics):
    return pltpu.CompilerParams(dimension_semantics=semantics or None, vmem_limit_bytes=mib << 20)


def hbm(array):
    return pltpu.with_memory_space_constraint(array, pltpu.HBM)


def whole(array):
    return pl.BlockSpec(array.shape, lambda *_: (0,) * array.ndim)


def cost(flops, moved):
    return pl.CostEstimate(flops=int(flops), bytes_accessed=int(moved), transcendentals=0)


def pack(obs, first, head, gains, chosen, slab, pad_acts):
    rows, features = obs.shape
    each, width = first.shape
    devices = width // slab
    acts = head.shape[0]
    mids = devices * each
    per = rows // features
    at = rows + mids + pad_acts
    total = at + -(-4 * per // 16) * 16

    def kernel(obs_ref, first_ref, head_ref, gains_ref, chosen_ref, out_ref):
        out_ref[:rows, :] = obs_ref[...]
        for b in range(devices):
            out_ref[rows + b * each : rows + (b + 1) * each, :] = first_ref[:, b * slab : (b + 1) * slab]
        out_ref[rows + mids :, :] = jnp.zeros((total - rows - mids, features), jnp.bfloat16)
        out_ref[rows + mids : rows + mids + acts, :] = head_ref[...]
        value = gains_ref[...]
        parts = []
        for _ in range(3):
            parts.append(value.astype(jnp.bfloat16))
            value = value - parts[-1].astype(jnp.float32)
        parts.append(chosen_ref[...].astype(jnp.float32).astype(jnp.bfloat16))
        for t, part in enumerate(parts):
            for r in range(per):
                row = at + t * per + r
                out_ref[row : row + 1, :] = part[:, r * features : (r + 1) * features]

    arrays = (obs, first, head, gains, chosen)
    return pl.pallas_call(
        kernel,
        name="pack",
        grid=(1,),
        in_specs=[whole(v) for v in arrays],
        out_specs=pl.BlockSpec((total, features), lambda i: (0, 0)),
        out_shape=pltpu.HBM((total, features), jnp.bfloat16),
        cost_estimate=cost(1 << 24, 1 << 20),
        compiler_params=params(6, "arbitrary"),
    )(*map(hbm, arrays))


def first_layer(order, scalars, pieces, theirs, rows, slab, near_blocks, pad_acts):
    count = len(pieces)
    devices = 2 * count
    features = pieces[0].shape[1]
    each = features // devices
    mids = devices * each
    width = devices * slab
    total = count * rows
    near_all = 2 * near_blocks

    def near_at(i):
        return (i // count) * near_blocks + jnp.minimum(i % count, near_blocks - 1)

    def kernel(order_ref, scalar_ref, *refs):
        live = scalar_ref[2] == 1
        piece_refs, theirs_ref = refs[:count], refs[count]
        h1_ref, h1t_ref, slope_ref, obst_ref, head_ref, cols = refs[count + 1 :]
        i = pl.program_id(0)

        def small(k, start, size):
            if k < count:
                return piece_refs[k][pl.ds(rows + start, size), :]
            return theirs_ref[k - count, pl.ds(start, size), :]

        @pl.when(live & (i == 0))
        def _():
            for k in range(devices):
                at = pl.multiple_of(order_ref[k] * each, each)
                lanes = pl.multiple_of(order_ref[k] * slab, slab)
                head_ref[:, pl.ds(lanes, slab)] = small(k, mids, pad_acts)
                for b in range(devices):
                    source = pl.multiple_of(order_ref[b] * each, each)
                    cols[b, pl.ds(at, each), :] = small(k, source, each)
            for p in range(count):
                block = piece_refs[p][:rows, :].astype(jnp.float32)
                obst_ref[:, p * rows : (p + 1) * rows] = block.T.astype(jnp.bfloat16)

        close = i % count < near_blocks

        @pl.when(live & close)
        def _():
            weights = cols[i]
            for p in range(count):
                at = slice(p * rows, (p + 1) * rows)
                obs = piece_refs[p][:rows, :]
                pre = dot(obs, weights)
                sig = sigmoid(pre)
                h1_ref[at, :] = (pre * sig).astype(jnp.bfloat16)
                slope_ref[at, :] = (sig * (1.0 + pre * (1.0 - sig))).astype(jnp.bfloat16)
                pre_t = dot(weights, obs, ((0,), (1,)))
                h1t_ref[:, at] = (pre_t * sigmoid(pre_t)).astype(jnp.bfloat16)

        @pl.when(live & jnp.logical_not(close))
        def _():
            weights = cols[i]
            for p in range(count):
                pre = dot(piece_refs[p][:rows, :], weights)
                h1_ref[p * rows : (p + 1) * rows, :] = (pre * sigmoid(pre)).astype(jnp.bfloat16)

    shape = lambda *s: jax.ShapeDtypeStruct(s, jnp.bfloat16)
    return pl.pallas_call(
        kernel,
        name="first_layer",
        grid_spec=pltpu.PrefetchScalarGridSpec(
            num_scalar_prefetch=2,
            grid=(devices,),
            in_specs=[whole(p) for p in pieces] + [whole(theirs)],
            out_specs=[
                pl.BlockSpec((total, slab), lambda i, *_: (0, i)),
                pl.BlockSpec((slab, total), lambda i, *_: (near_at(i), 0)),
                pl.BlockSpec((total, slab), lambda i, *_: (0, near_at(i))),
                pl.BlockSpec((features, total), lambda i, *_: (0, 0)),
                pl.BlockSpec((pad_acts, width), lambda i, *_: (0, 0)),
            ],
            scratch_shapes=[pltpu.VMEM((devices, features, slab), jnp.bfloat16)],
        ),
        out_shape=[
            shape(total, width),
            shape(near_all * slab, total),
            pltpu.HBM((total, near_all * slab), jnp.bfloat16),
            pltpu.HBM((features, total), jnp.bfloat16),
            shape(pad_acts, width),
        ],
        cost_estimate=cost(2 * total * features * width * 2, 30 << 20),
        compiler_params=params(20, "arbitrary"),
    )(order, scalars, *map(hbm, pieces), theirs)


def second_layer(scalars, hidden1, own, pieces, theirs, head, logits, hidden2, start, inner, cut):
    total, width = hidden1.shape
    slab = own.shape[0]
    pad_acts = head.shape[0]
    tile = min(512, total)
    first = logits is None
    sub = 256
    q = start // cut

    def kernel(scalar_ref, h1_ref, own_ref, *refs):
        live = scalar_ref[2] == 1
        piece_refs = refs[: len(pieces)]
        theirs_ref, head_ref = refs[len(pieces) : len(pieces) + 2]
        rest = refs[len(pieces) + 2 :]
        logits_in = None if first else rest[0]
        h2_ref, slope_ref, logits_ref, weights = rest[0 if first else 2 :]

        @pl.when(live & (pl.program_id(0) == 0))
        def _():
            weights[:slab] = own_ref[...]
            for k, piece in enumerate(piece_refs):
                weights[(k + 1) * slab : (k + 2) * slab] = piece[...]
            weights[(len(pieces) + 1) * slab :] = theirs_ref[...]

        @pl.when(live)
        def _():
            for r in range(0, tile, sub):
                pre = dot(h1_ref[r : r + sub, :], weights[...])
                sig = sigmoid(pre)
                hidden = (pre * sig).astype(jnp.bfloat16)
                h2_ref[r : r + sub, :] = hidden
                slope_ref[r : r + sub, :] = (sig * (1.0 + pre * (1.0 - sig))).astype(jnp.bfloat16)
                part = dot(hidden, head_ref[...], ((1,), (1,)))
                logits_ref[r : r + sub, :] = part if first else part + logits_in[r : r + sub, :]

    row = lambda size: pl.BlockSpec((tile, size), lambda i: (i, 0))
    return pl.pallas_call(
        kernel,
        name="second_layer",
        grid=(total // tile,),
        in_specs=[pl.BlockSpec(memory_space=pltpu.SMEM), row(width), pl.BlockSpec((slab, cut), lambda i: (0, q))]
        + [pl.BlockSpec((slab, cut), lambda i: (0, inner))] * len(pieces)
        + [pl.BlockSpec((theirs.shape[0], cut), lambda i: (0, inner)), pl.BlockSpec((pad_acts, cut), lambda i: (0, q))]
        + ([] if first else [row(pad_acts), pl.BlockSpec(memory_space=pltpu.HBM)]),
        out_specs=[pl.BlockSpec((tile, cut), lambda i: (i, q)), row(cut), row(pad_acts)],
        out_shape=[
            pltpu.HBM((total, width), jnp.bfloat16),
            jax.ShapeDtypeStruct((total, cut), jnp.bfloat16),
            jax.ShapeDtypeStruct((total, pad_acts), jnp.float32),
        ],
        scratch_shapes=[pltpu.VMEM((width, cut), jnp.bfloat16)],
        input_output_aliases={} if first else {len(pieces) + 6: 0},
        cost_estimate=cost(2 * total * width * cut, 16 << 20),
        compiler_params=params(12 + (8 * width * cut >> 20), "arbitrary"),
    )(scalars, hidden1, hbm(own), *pieces, theirs, head, *([] if first else [logits, hbm(hidden2)]))


def policy(logits_raw, pieces, at, acts, batch):
    total, pad_acts = logits_raw.shape
    count = len(pieces)
    features = pieces[0].shape[1]
    per = total // count // features
    size = pieces[0].shape[0] - at

    def kernel(raw_ref, *refs):
        label_refs = refs[:count]
        graw_ref, graw_t_ref, score_ref = refs[count:]
        raw = raw_ref[...].T
        blocks = [ref[...].astype(jnp.float32) for ref in label_refs]
        part = lambda t: jnp.concatenate(
            [block[t * per + r : t * per + r + 1, :] for block in blocks for r in range(per)], axis=1
        )
        gains, chosen = part(0) + part(1) + part(2), part(3).astype(jnp.int32)
        at = lax.broadcasted_iota(jnp.int32, raw.shape, 0)
        live = at < acts
        squash = jnp.tanh(raw / CAP)
        logits = CAP * squash
        mass = jnp.sum(jnp.where(live, jnp.exp(logits), 0.0), axis=0, keepdims=True)
        logp = logits - jnp.log(mass)
        onehot = at == chosen
        taken = jnp.sum(jnp.where(onehot, logp, 0.0), axis=0, keepdims=True)
        score_ref[...] = jnp.sum(gains * taken, axis=1, keepdims=True) / batch
        grad = -(gains / batch) * (onehot.astype(jnp.float32) - jnp.exp(logp)) * (1.0 - squash * squash)
        grad = jnp.where(live, grad, 0.0)
        graw_t_ref[...] = grad.astype(jnp.bfloat16)
        graw_ref[...] = grad.T.astype(jnp.bfloat16)

    return pl.pallas_call(
        kernel,
        name="policy",
        grid=(1,),
        in_specs=[whole(logits_raw)] + [pl.BlockSpec((size, features), lambda i: (at // size, 0))] * count,
        out_specs=[
            pl.BlockSpec((total, pad_acts), lambda i: (0, 0)),
            pl.BlockSpec((pad_acts, total), lambda i: (0, 0)),
            pl.BlockSpec((1, 1), lambda i: (0, 0)),
        ],
        out_shape=[
            jax.ShapeDtypeStruct((total, pad_acts), jnp.bfloat16),
            jax.ShapeDtypeStruct((pad_acts, total), jnp.bfloat16),
            jax.ShapeDtypeStruct((1, 1), jnp.float32),
        ],
        cost_estimate=cost(1 << 28, 2 << 20),
        compiler_params=params(10, "arbitrary"),
    )(logits_raw, *map(hbm, pieces))


def middle_grad(scalars, graw, head, slopes, hidden1_t, start, cut):
    total, pad_acts = graw.shape
    near_rows = hidden1_t.shape[0]
    kept = near_rows // 2
    tile = min(256, kept)
    steps = near_rows // tile
    parts = len(slopes)
    span = parts * cut

    def kernel(scalar_ref, graw_ref, head_ref, *refs):
        live = scalar_ref[2] == 1
        slope_refs = refs[:parts]
        h1t_ref, g2_ref, keep_ref, give_ref = refs[parts:]
        i = pl.program_id(0)

        @pl.when(live & (i == 0))
        def _():
            for p in range(parts):
                lanes = slice(p * cut, (p + 1) * cut)
                for r in range(0, total, 256):
                    g2 = dot(graw_ref[r : r + 256, :], head_ref[:, lanes]) * slope_refs[p][r : r + 256, :].astype(jnp.float32)
                    g2_ref[r : r + 256, lanes] = g2.astype(jnp.bfloat16)

        @pl.when(live & (i < steps // 2))
        def _():
            give_ref[...] = dot(h1t_ref[...], g2_ref[...]).astype(jnp.bfloat16)

        @pl.when(live & (i >= steps // 2))
        def _():
            keep_ref[...] = dot(h1t_ref[...], g2_ref[...])

    turn = lambda i: (i + steps // 2) % steps
    return pl.pallas_call(
        kernel,
        name="middle_grad",
        grid=(steps,),
        in_specs=[pl.BlockSpec(memory_space=pltpu.SMEM), whole(graw), pl.BlockSpec((pad_acts, span), lambda i: (0, start // span))]
        + [whole(v) for v in slopes]
        + [pl.BlockSpec((tile, total), lambda i: (turn(i), 0))],
        out_specs=[
            pl.BlockSpec((total, span), lambda i: (0, 0)),
            pl.BlockSpec((tile, span), lambda i: (jnp.maximum(i - steps // 2, 0), 0)),
            pl.BlockSpec((tile, span), lambda i: (jnp.minimum(i, steps // 2 - 1), 0)),
        ],
        out_shape=[
            pltpu.HBM((total, span), jnp.bfloat16),
            jax.ShapeDtypeStruct((kept, span), jnp.float32),
            pltpu.HBM((kept, span), jnp.bfloat16),
        ],
        cost_estimate=cost(2 * total * near_rows * span, 16 << 20),
        compiler_params=params(24, "arbitrary"),
    )(scalars, graw, head, *slopes, hidden1_t)


def head_grad(scalars, graw_t, hidden2):
    pad_acts, total = graw_t.shape
    side = hidden2.shape[1] // 2
    block = min(512, side)

    def kernel(scalar_ref, graw_t_ref, h2_ref, out_ref):
        out_ref[...] = dot(graw_t_ref[...], h2_ref[...])

    return pl.pallas_call(
        kernel,
        name="head_grad",
        grid_spec=pltpu.PrefetchScalarGridSpec(
            num_scalar_prefetch=1,
            grid=(side // block,),
            in_specs=[
                pl.BlockSpec((pad_acts, total), lambda i, _: (0, 0)),
                pl.BlockSpec((total, block), lambda i, s: (0, s[1] * (side // block) + i)),
            ],
            out_specs=pl.BlockSpec((pad_acts, block), lambda i, _: (0, i)),
        ),
        out_shape=jax.ShapeDtypeStruct((pad_acts, side), jnp.float32),
        cost_estimate=cost(2 * total * side * 256, 6 << 20),
        compiler_params=params(10, "arbitrary"),
    )(scalars, graw_t, hbm(hidden2))


def middle_update(rate, keep, got, own, near_pieces, group, span, cut):
    slab = own.shape[0]
    per = span // cut
    blocks = 1 + len(near_pieces[0])
    flat = [p for chunk in near_pieces for p in chunk]

    def kernel(rate_ref, keep_ref, got_ref, own_ref, *refs):
        flat_refs, out_refs = refs[: len(flat)], refs[len(flat) :]
        rate = rate_ref[0:1, 0:1]
        for s in reversed(range(blocks)):
            for p in range(per):
                lanes, at = slice(p * cut, (p + 1) * cut), slice(s * slab, (s + 1) * slab)
                weight = own_ref[:, lanes] if s == 0 else flat_refs[p * (blocks - 1) + s - 1][...]
                total = keep_ref[at, lanes] + got_ref[at, lanes].astype(jnp.float32)
                out_refs[s][:, lanes] = (weight.astype(jnp.float32) - rate * total).astype(jnp.bfloat16)

    return pl.pallas_call(
        kernel,
        name="middle_update",
        grid=(1,),
        in_specs=[whole(rate), whole(keep), whole(got)]
        + [pl.BlockSpec((slab, span), lambda i: (0, group))]
        + [whole(p) for p in flat],
        out_specs=[pl.BlockSpec((slab, span), lambda i: (0, 0))] * blocks,
        out_shape=[pltpu.HBM((slab, span), jnp.bfloat16)] * blocks,
        cost_estimate=cost(1 << 27, 4 << 20),
        compiler_params=params(16, "arbitrary"),
    )(rate, keep, got, hbm(own), *flat)


def gather_small(scalars, order, keep, got, side, score, first_rows, slab, half):
    count = 2 * half
    devices = 2 * count
    mids = devices * first_rows
    pad_acts = side.shape[0]
    acts_at = mids + pad_acts

    def kernel(scalar_ref, order_ref, keep_ref, got_ref, side_ref, score_ref, mine_ref, sent_ref):
        core = scalar_ref[0]
        for target, which in ((sent_ref, 1 - core), (mine_ref, core)):
            for j in range(half):
                base = pl.multiple_of(j * 2 * first_rows + which * first_rows, first_rows)
                for k in range(devices):
                    source = got_ref if (k // half) % 2 else keep_ref
                    lanes = ((k // count) * half + k % half) * slab
                    at = pl.multiple_of(order_ref[k] * first_rows, first_rows)
                    target[j, pl.ds(at, first_rows), :] = source[pl.ds(base, first_rows), lanes : lanes + slab]
                cols = pl.multiple_of((j * 2 + which) * slab, slab)
                target[j, mids:acts_at, :] = side_ref[:, pl.ds(cols, slab)].astype(jnp.bfloat16)
        value = jnp.broadcast_to(score_ref[...], (1, slab))
        for part in range(3):
            piece = value.astype(jnp.bfloat16)
            sent_ref[0, acts_at - 3 + part : acts_at - 2 + part, :] = piece
            value = value - piece.astype(jnp.float32)

    shape = jax.ShapeDtypeStruct((half, acts_at, slab), jnp.bfloat16)
    smem = pl.BlockSpec(memory_space=pltpu.SMEM)
    arrays = [keep, got, side, score]
    return pl.pallas_call(
        kernel,
        name="gather_small",
        grid=(1,),
        in_specs=[smem, smem] + [whole(v) for v in arrays],
        out_specs=[whole(shape)] * 2,
        out_shape=[shape, pltpu.HBM(shape.shape, shape.dtype)],
        cost_estimate=cost(1 << 26, 2 << 20),
        compiler_params=params(8, "arbitrary"),
    )(scalars, order, *arrays)


def small_update(scalars, rate, mine, got, weights, score, at_row):
    half, rows, slab = mine.shape

    def kernel(scalar_ref, rate_ref, mine_ref, got_ref, *refs):
        weight_refs = refs[:half]
        score_ref, fitness_ref = refs[half], refs[half + 1]
        out_refs = refs[half + 2 :]
        rate, high = rate_ref[0:1, 0:1], scalar_ref[1]
        fitness = jnp.broadcast_to(score_ref[...], (1, slab))
        for part in range(3):
            fitness = fitness + got_ref[0, rows - 3 + part : rows - 2 + part, :].astype(jnp.float32)
        fitness_ref[...] = fitness[:, :1]
        for s in range(half):
            at = jnp.where(high == 1, s, half - 1 - s)
            total = mine_ref[at].astype(jnp.float32) + got_ref[at].astype(jnp.float32)
            out_refs[s][...] = (weight_refs[s][at_row : at_row + rows, :].astype(jnp.float32) - rate * total).astype(jnp.bfloat16)
            value = fitness
            for part in range(3):
                piece = value.astype(jnp.bfloat16)
                out_refs[s][rows - 3 + part : rows - 2 + part, :] = piece
                value = value - piece.astype(jnp.float32)

    smem = pl.BlockSpec(memory_space=pltpu.SMEM)
    return pl.pallas_call(
        kernel,
        name="small_update",
        grid=(1,),
        in_specs=[smem] + [whole(v) for v in (rate, mine, got, *weights, score)],
        out_specs=[pl.BlockSpec((1, 1), lambda i: (0, 0))] + [pl.BlockSpec((rows, slab), lambda i: (0, 0))] * half,
        out_shape=[jax.ShapeDtypeStruct((1, 1), jnp.float32)] + [pltpu.HBM((rows, slab), jnp.bfloat16)] * half,
        cost_estimate=cost(1 << 26, 2 << 20),
        compiler_params=params(8, "arbitrary"),
    )(scalars, rate, mine, got, *map(hbm, weights), score)


def input_grad(scalars, grads, own, near_pieces, theirs, slope, obs_t):
    total = grads[0].shape[0]
    slab, width = own.shape
    near_rows = slope.shape[1]
    kept = near_rows // 2
    features = obs_t.shape[0]
    groups = len(grads)
    chunks = len(theirs)
    side = features // 2
    tile = min(512, total)
    cuts = [v.shape[1] for v in theirs]
    starts = [sum(cuts[:q]) for q in range(chunks)]
    flat = [p for chunk in near_pieces for p in chunk]
    per = len(flat) // chunks

    def kernel(scalar_ref, *refs):
        g_refs, refs = refs[:groups], refs[groups:]
        own_ref, refs = refs[0], refs[1:]
        flat_refs, refs = refs[: len(flat)], refs[len(flat) :]
        theirs_refs, refs = refs[:chunks], refs[chunks:]
        slope_ref, obst_ref, keep_ref, give_ref, weights, total_ref = refs
        i = pl.program_id(0)
        live = scalar_ref[2] == 1

        @pl.when(live & (i == 0))
        def _():
            weights[:slab] = own_ref[...]
            for q in range(chunks):
                lanes = slice(starts[q], starts[q] + cuts[q])
                for k in range(per):
                    weights[(k + 1) * slab : (k + 2) * slab, lanes] = flat_refs[q * per + k][...]
                weights[kept:, lanes] = theirs_refs[q][...]
            total_ref[...] = jnp.zeros_like(total_ref)

        @pl.when(live)
        def _():
            g2 = jnp.concatenate([g[...] for g in g_refs], axis=1)
            back = dot(g2, weights[...], ((1,), (1,)))
            grad = (back * slope_ref[...].astype(jnp.float32)).astype(jnp.bfloat16)
            total_ref[...] += dot(obst_ref[...], grad)

        @pl.when(live & (i == pl.num_programs(0) - 1))
        def _():
            high = scalar_ref[1]
            keep_ref[...] = total_ref[pl.ds(pl.multiple_of(high * side, side), side), :].astype(jnp.bfloat16)
            give_ref[...] = total_ref[pl.ds(pl.multiple_of((1 - high) * side, side), side), :].astype(jnp.bfloat16)

    return pl.pallas_call(
        kernel,
        name="input_grad",
        grid=(total // tile,),
        in_specs=[pl.BlockSpec(memory_space=pltpu.SMEM)]
        + [pl.BlockSpec((tile, g.shape[1]), lambda i: (i, 0)) for g in grads]
        + [whole(own)]
        + [whole(p) for p in flat]
        + [pl.BlockSpec((kept, cut), lambda i: (0, 0)) for cut in cuts]
        + [pl.BlockSpec((tile, near_rows), lambda i: (i, 0)), pl.BlockSpec((features, tile), lambda i: (0, i))],
        out_specs=[pl.BlockSpec((side, near_rows), lambda i: (0, 0))] * 2,
        out_shape=[
            jax.ShapeDtypeStruct((side, near_rows), jnp.bfloat16),
            pltpu.HBM((side, near_rows), jnp.bfloat16),
        ],
        scratch_shapes=[
            pltpu.VMEM((near_rows, width), jnp.bfloat16),
            pltpu.VMEM((features, near_rows), jnp.float32),
        ],
        cost_estimate=cost(2 * total * near_rows * width, 20 << 20),
        compiler_params=params(34, "arbitrary"),
    )(scalars, *map(hbm, grads), hbm(own), *map(hbm, flat), *map(hbm, theirs), hbm(slope), hbm(obs_t))


def settings(numbers, log_rate, copy_from, perturb, devices):
    members = log_rate.shape[0]

    def kernel(numbers_ref, log_rate_ref, copy_ref, perturb_ref, order_ref, scalars_ref, rate_ref, flag_ref, next_ref):
        for k in range(devices):
            order_ref[k] = numbers_ref[k]
        for k in range(3):
            scalars_ref[k] = numbers_ref[devices + k]
        member = numbers_ref[devices + 3]
        rate_ref[...] = jnp.exp(jnp.full(rate_ref.shape, log_rate_ref[member], jnp.float32))
        taken = copy_ref[member] == 1
        flag_ref[0] = taken.astype(jnp.int32)
        source = jnp.where(taken, lax.rem(member + members - 1, members), member)
        pick = perturb_ref[member]
        offset = jnp.where(pick == 0, -0.2, jnp.where(pick == 1, 0.0, 0.2)).astype(jnp.float32)
        next_ref[...] = jnp.full(next_ref.shape, log_rate_ref[source] + offset, jnp.float32)

    smem = pl.BlockSpec(memory_space=pltpu.SMEM)
    vmem = pl.BlockSpec(memory_space=pltpu.VMEM)
    ints = lambda n: jax.ShapeDtypeStruct((n,), jnp.int32)
    return pl.pallas_call(
        kernel,
        name="settings",
        in_specs=[smem] * 4,
        out_specs=[smem, smem, vmem, smem, vmem],
        out_shape=[
            ints(devices),
            ints(3),
            jax.ShapeDtypeStruct((8, 128), jnp.float32),
            ints(1),
            jax.ShapeDtypeStruct((1, 1), jnp.float32),
        ],
        cost_estimate=cost(1 << 10, 1 << 10),
        compiler_params=params(4),
    )(numbers, log_rate, copy_from, perturb)


def hub_body(observations, returns, actions, w_input, w_middle, w_head, log_rate, copy_from, perturb):
    obs = observations[0]
    own_first, own_middle, own_head = w_input[0], w_middle[0], w_head[0]
    devices = lax.axis_size("dp")
    half = devices // 4
    count = 2 * half
    rows, _ = obs.shape
    first_rows, width = own_first.shape
    slab = own_middle.shape[0]
    acts = own_head.shape[1]
    pad_acts = -(-(acts + 3) // 32) * 32
    batch = rows * devices
    mids = devices * first_rows
    cuts = [width // part for part in PARTS]
    starts = [sum(cuts[:q]) for q in range(len(cuts))]
    cut = min(cuts)
    place = lax.axis_index("dp")
    core = place % 2
    chip = place // 2
    high = (chip >= half).astype(jnp.int32)
    member = lax.axis_index("pop")
    members = lax.axis_size("pop")
    ring = [(i, (i + 1) % members) for i in range(members)]

    def side(step, upper):
        return half + step if upper else half - 1 - step

    def route(step, crossing, back=False):
        pairs = []
        for upper in (False, True):
            hub = side(0, upper != crossing)
            end = side(step, upper)
            pairs += [(2 * end + c, 2 * hub + c) for c in range(2)]
        return [(b, a) for a, b in pairs] if back else pairs

    def near(value, step):
        return lax.ppermute(value, "dp", route(step, False))

    def far(value, step):
        return lax.ppermute(value, "dp", route(step, True))

    def outward(value, step):
        return lax.ppermute(value, "dp", route(step, False, True))

    def partner(value):
        return lax.ppermute(value, "dp", [(i, i ^ 1) for i in range(devices)])

    def shifted(value):
        return lax.ppermute(value, "pop", ring)

    slots = jnp.arange(devices, dtype=jnp.int32)
    upper = high ^ ((slots // half) % 2)
    order = 2 * jnp.where(upper == 1, half + slots % half, half - 1 - slots % half) + (core ^ (slots // count))

    hub = ((chip == half) | (chip == half - 1)).astype(jnp.int32)
    numbers = jnp.concatenate([order, jnp.stack([core, high, hub, member])]).astype(jnp.int32)
    order, scalars, rate, flag, next_rate = settings(numbers, log_rate, copy_from, perturb, devices)

    def column(value):
        out = []
        for s in range(1, half):
            out.append(near(value, s))
        for s in range(half):
            out.append(far(value, s))
        return out

    labels_at = rows + mids + pad_acts
    packed = pack(obs, own_first, own_head.T, returns, actions, slab, pad_acts)
    pieces = [packed] + column(packed)
    columns = [own_middle[:, start : start + cut] for start, cut in zip(starts, cuts)]
    middle_pieces = [column(columns[q]) for q in range(len(cuts))]
    theirs_small = partner(jnp.stack([p[rows:labels_at] for p in pieces]))
    hidden1, near_t, slope1, obs_t, head = first_layer(order, scalars, pieces, theirs_small, rows, slab, half, pad_acts)

    logits = None
    hidden2, slope2, theirs = None, [], []
    for q in range(len(cuts)):
        mine = jnp.concatenate([columns[q]] + middle_pieces[q], axis=0)
        theirs.append(partner(mine))
        for inner in range(cuts[q] // cut):
            start = starts[q] + inner * cut
            hidden2, slope, logits = second_layer(
                scalars, hidden1, own_middle, middle_pieces[q], theirs[q], head, logits, hidden2, start, inner, cut
            )
            slope2.append(slope)

    grad_raw, grad_raw_t, score = policy(logits, pieces, labels_at, acts, batch)

    distance = jnp.where(high == 1, chip - half, half - 1 - chip)

    def home(blocks):
        out = blocks[0]
        for s in range(1, half):
            moved = outward(blocks[s], s)
            out = jnp.where(distance == s, moved, out)
        return out

    flag = flag[0] == 1

    near_w = [m[: half - 1] for m in middle_pieces]
    span = width // GROUPS
    out_middle, grads = [], []
    for g in range(GROUPS):
        which = [q for q in range(len(cuts)) if starts[q] // span == g]
        parts = range(g * span // cut, (g + 1) * span // cut)
        g2, keep, give = middle_grad(scalars, grad_raw, head, [slope2[p] for p in parts], near_t, g * span, cut)
        got = partner(give)
        new = middle_update(rate, keep, got, own_middle, [near_w[q] for q in which], g, span, cuts[which[0]])
        new = home(new)
        moved = shifted(new)
        out_middle.append(jnp.where(flag, moved, new))
        grads.append(g2)
    out_middle = jnp.concatenate(out_middle, axis=1)

    keep, give = input_grad(scalars, grads, own_middle, near_w, theirs, slope1, obs_t)
    got = far(give, 0)
    head_term = head_grad(scalars, grad_raw_t, hidden2)
    mine, sent = gather_small(scalars, order, keep, got, head_term, score, first_rows, slab, half)
    got = partner(sent)
    fitness, *new_small = small_update(scalars, rate, mine, got, pieces[:half], score, rows)
    new_small = home(new_small)
    fitness = jnp.where(
        distance == 0, fitness, jnp.sum(new_small[-3:, :1].astype(jnp.float32), axis=0, keepdims=True)
    )
    moved = shifted(new_small)
    out_small = jnp.where(flag, moved, new_small)
    out_first = out_small[:mids].reshape(devices, first_rows, slab).swapaxes(0, 1).reshape(first_rows, width)
    out_head = out_small[mids : mids + acts].T

    return (
        out_first[None],
        out_middle[None],
        out_head[None],
        next_rate.reshape(1),
        fitness.reshape(1),
    )


def hub_step(*arrays):
    return hub_body(*arrays)


def shifted(block, axis, distance):
    devices = range(lax.axis_size(axis))
    route = [((i - distance) % len(devices), i) for i in devices]
    return lax.ppermute(block, axis, route)


def local(observations, returns, actions, w_input, w_middle, w_head, log_rate, copy_from, perturb):
    obs = observations[0]
    gains = returns[0]
    chosen = actions[0]
    own_first = w_input[0]
    own_middle = w_middle[0]
    own_head = w_head[0]
    rows = obs.shape[0]
    batch = rows * lax.axis_size("dp")
    first, head = (
        lax.all_gather(own_first, "dp", axis=0, tiled=True),
        lax.all_gather(own_head, "dp", axis=0, tiled=True),
    )
    pre1 = jnp.dot(obs, first, preferred_element_type=jnp.float32)
    hidden1 = jax.nn.silu(pre1).astype(jnp.bfloat16)
    columns = hidden1
    pre2 = jnp.dot(
        columns,
        lax.all_gather(own_middle, "dp", axis=0, tiled=True),
        preferred_element_type=jnp.float32,
    )
    hidden2 = jax.nn.silu(pre2).astype(jnp.bfloat16)
    squash = jnp.tanh(jnp.dot(hidden2, head, preferred_element_type=jnp.float32) / CAP)
    logits = CAP * squash
    logp = logits - jnp.log(jnp.sum(jnp.exp(logits), axis=1, keepdims=True))
    onehot = (chosen[:, None] == lax.broadcasted_iota(jnp.int32, logits.shape, 1)).astype(
        jnp.float32
    )
    taken = jnp.sum(logp * onehot, axis=1)
    fitness = lax.psum(jnp.sum(gains * taken) / batch, "dp")
    grad_raw = (
        -(gains / batch)[:, None] * (onehot - jnp.exp(logp)) * (1.0 - squash * squash)
    ).astype(jnp.bfloat16)
    head_term = contract_rows(hidden2, grad_raw)
    grad_pre2 = (contract_cols(grad_raw, head) * silu_slope(pre2)).astype(jnp.bfloat16)
    columns = hidden1
    grad_middle = lax.psum_scatter(
        contract_rows(columns, grad_pre2).astype(jnp.bfloat16),
        "dp",
        scatter_dimension=0,
        tiled=True,
    ).astype(jnp.float32)
    member = lax.axis_index("pop")
    members = lax.axis_size("pop")
    rate = jnp.exp(lax.dynamic_index_in_dim(log_rate, member, keepdims=False))
    new_middle = (own_middle.astype(jnp.float32) - rate * grad_middle).astype(jnp.bfloat16)
    back = contract_cols(grad_pre2, lax.all_gather(own_middle, "dp", axis=0, tiled=True))
    grad_pre1 = (back * silu_slope(pre1)).astype(jnp.bfloat16)
    input_term = contract_rows(obs, grad_pre1)
    grad_first, grad_head = (
        lax.psum_scatter(
            input_term.astype(jnp.bfloat16), "dp", scatter_dimension=0, tiled=True
        ).astype(jnp.float32),
        lax.psum_scatter(
            head_term.astype(jnp.bfloat16), "dp", scatter_dimension=0, tiled=True
        ).astype(jnp.float32),
    )
    new_first = (own_first.astype(jnp.float32) - rate * grad_first).astype(jnp.bfloat16)
    new_head = (own_head.astype(jnp.float32) - rate * grad_head).astype(jnp.bfloat16)
    moved_first, moved_middle, moved_head = shifted((new_first, new_middle, new_head), "pop", 1)
    flag = lax.dynamic_index_in_dim(copy_from, member, keepdims=False) == 1
    out_first = jnp.where(flag, moved_first, new_first)
    out_middle = jnp.where(flag, moved_middle, new_middle)
    out_head = jnp.where(flag, moved_head, new_head)
    source = jnp.where(flag, (member + members - 1) % members, member)
    pick = lax.dynamic_index_in_dim(perturb, member, keepdims=False)
    offset = jnp.where(pick == 0, -0.2, jnp.where(pick == 1, 0.0, 0.2)).astype(jnp.float32)
    next_rate = lax.dynamic_index_in_dim(log_rate, source, keepdims=False) + offset
    return (
        out_first[None],
        out_middle[None],
        out_head[None],
        next_rate.reshape(1),
        fitness.reshape(1),
    )


def solution(mesh):
    in_specs = (
        P("pop", "dp", None),
        P("pop", "dp"),
        P("pop", "dp"),
        P("pop", "dp", None),
        P("pop", "dp", None),
        P("pop", "dp", None),
        P(),
        P(),
        P(),
    )
    out_specs = (
        P("pop", "dp", None),
        P("pop", "dp", None),
        P("pop", "dp", None),
        P("pop"),
        P("pop"),
    )

    def step(*arrays):
        observations, w_middle = arrays[0], arrays[4]
        small = observations.shape[1] // 2 <= w_middle.shape[2] and mesh.shape["dp"] % 4 == 0
        small = small and arrays[3].shape[1] * mesh.shape["dp"] == w_middle.shape[2]
        body = hub_step if small else local
        step = jax.shard_map(body, mesh=mesh, in_specs=in_specs, out_specs=out_specs, check_vma=False)
        return step(*arrays)

    return step
```
